32 devices in a mesh: gx: 4 (over y, x), gy: 8 (over z, core).
Axes of the slice: x: 2, y: 2, z: 4, core: 2. Of those that a mesh axis runs over, the one named last changes fastest.
Arguments:
- cotangent: float32 [128, 512, 128], P('gx', 'gy'), may hold values from -6 to 6
- speed: float32 [3, 128, 512, 128], P(None, 'gx', 'gy'), may hold values from 0.05 to 0.45
- coeff: float32 [3, 128, 512, 128], P(None, 'gx', 'gy'), may hold values from 0.3 to 3
- dirs: int32 [3, 128, 512], P(None, 'gx', 'gy'), may hold values from 0 to 1
Outputs:
- grad: float32 [128, 512, 128], P('gx', 'gy')
The draws below stay inside these ranges and needn't reach their ends.
Inputs may be any that keep to these rules, and one draw needn't show every extreme that they name: `dirs`: 0 means the lower cell of a face is upwind, 1 the upper cell.
All inputs are finite; a program needn't handle non-finite values.
Results may differ from the reference program's by a relative error of at most 0.0003.
Values sent between devices are 32-bit elements; how exact they have to be, the bound alone decides.
A program may use at most 128 MiB of HBM per device.

```python
import math
import jax
import jax.numpy as jnp
from jax import lax

NZ = 128
ITERS = 2
NX = 128
NY = 512


def plant(array, rng, smallest, top_value):
    index_at = [jax.random.randint(jax.random.fold_in(rng, axis), (), 0, length) for axis, length in enumerate(array.shape)]
    main_axis = array.shape.index(max(array.shape))
    next_to = index_at[:main_axis] + [(index_at[main_axis] + 1) % array.shape[main_axis]] + index_at[main_axis + 1:]
    return array.at[tuple(index_at)].set(smallest).at[tuple(next_to)].set(top_value)


def shard_levels(own_key, shape, pieces, smallest, top_value):
    gain = 1.0
    for dim, parts in pieces:
        steps = jax.random.uniform(jax.random.fold_in(jax.random.fold_in(own_key, 6), dim), (parts,), jnp.float32, smallest / len(pieces), top_value / len(pieces))
        gain = gain * jnp.repeat(jnp.exp(steps), shape[dim] // parts).reshape((-1,) + (1,) * (len(shape) - 1 - dim))
    return gain


def scatter_about(rng, dims, width, limit, shards=(), held_as=jnp.bfloat16):
    drawn = width * jax.random.normal(rng, dims, jnp.float32)
    if shards:
        drawn = drawn * shard_levels(rng, dims, shards, -0.22, 0.18)
    return jnp.clip(drawn, -limit, limit).astype(held_as)


def setup_inputs(seed: int = 0) -> dict:
    seeds = jax.random.split(jax.random.key(seed), 5)
    return {
        "cotangent": scatter_about(seeds[0], (NX, NY, NZ), 1.0, 6.0, ((0, 4), (1, 8)), jnp.float32),
        "speed": jnp.clip(jnp.exp(math.log(0.45) - 2.1972245 * jax.random.uniform(seeds[1], (3, NX, NY, NZ), jnp.float32) ** shard_levels(seeds[1], (3, NX, NY, NZ), ((1, 4), (2, 8)), -0.2, 0.2)), 0.05, 0.45),
        "coeff": jnp.clip(jnp.exp(math.log(3.0) - 2.3025851 * jax.random.uniform(seeds[2], (3, NX, NY, NZ), jnp.float32) ** shard_levels(seeds[2], (3, NX, NY, NZ), ((1, 4), (2, 8)), -0.2, 0.2)), 0.3, 3.0),
        "dirs": plant(jax.random.randint(seeds[3], (3, NX, NY), 0, 2), jax.random.fold_in(seeds[3], 1), 0, 1).astype(jnp.int32),
    }


explicit_table = ((0.0, 0.0, 0.0, 0.0), (0.5, 0.0, 0.0, 0.0), (0.25, 0.5, 0.0, 0.0), (0.2, 0.3, 0.5, 0.0))
implicit_table = ((0.0, 0.0, 0.0, 0.0), (0.25, 0.25, 0.0, 0.0), (0.25, 0.25, 0.25, 0.0), (0.15, 0.35, 0.25, 0.25))
section_weights = (0.15, 0.35, 0.25, 0.25)
implicit_diagonal = 0.25
step_length = 1.0


def local_ahead(values, dimension):
    tail = lax.slice_in_dim(values, 1, values.shape[dimension], axis=dimension)
    return jnp.concatenate([tail, jnp.zeros_like(lax.slice_in_dim(values, 0, 1, axis=dimension))], dimension)


def local_behind(values, dimension):
    head = lax.slice_in_dim(values, 0, values.shape[dimension] - 1, axis=dimension)
    return jnp.concatenate([jnp.zeros_like(lax.slice_in_dim(values, 0, 1, axis=dimension)), head], dimension)


def transposed(advected, diffused, velocity, coeff):
    total = jnp.zeros_like(diffused)
    for dimension in range(3):
        flux = coeff[dimension] * (local_ahead(diffused, dimension) - diffused)
        total = total + flux - local_behind(flux, dimension)
        if advected is not None:
            moved = velocity[dimension] * (local_ahead(advected, dimension) - advected)
            upwind_here = velocity[dimension] > 0
            total = total + jnp.where(upwind_here, moved, 0.0)
            total = total + local_behind(jnp.where(upwind_here, 0.0, moved), dimension)
    return total


def solve_section(rhs, velocity, coeff):
    solution = jnp.zeros_like(rhs)
    residual = rhs
    direction = rhs
    norm_now = jnp.sum(residual * residual)
    for iteration in range(ITERS):
        image = direction - implicit_diagonal * step_length * transposed(None, direction, velocity, coeff)
        alpha = norm_now / jnp.sum(direction * image)
        solution = solution + alpha * direction
        residual = residual - alpha * image
        norm_next = jnp.sum(residual * residual)
        direction = residual + (norm_next / norm_now) * direction
        norm_now = norm_next
    return solution


def reference(cotangent, speed, coeff, dirs):
    signs = (1 - 2 * dirs).astype(jnp.float32)
    velocity = speed * signs[..., None]
    section_adjoints = [None, None, None, None]
    for section_index in (3, 2, 1, 0):
        advected = step_length * section_weights[section_index] * cotangent
        diffused = step_length * section_weights[section_index] * cotangent
        for later in range(section_index + 1, 4):
            advected = advected + step_length * explicit_table[later][section_index] * section_adjoints[later]
            diffused = diffused + step_length * implicit_table[later][section_index] * section_adjoints[later]
        source = transposed(advected, diffused, velocity, coeff)
        if section_index > 0:
            section_adjoints[section_index] = solve_section(source, velocity, coeff)
        else:
            section_adjoints[section_index] = source
    return cotangent + section_adjoints[0] + section_adjoints[1] + section_adjoints[2] + section_adjoints[3]
```

```python
import functools

import jax
import jax.numpy as jnp
from jax import lax
from jax.experimental import pallas as pl
from jax.experimental.pallas import tpu as pltpu
from jax.sharding import PartitionSpec as P

explicit_table = (
    (0.0, 0.0, 0.0, 0.0),
    (0.5, 0.0, 0.0, 0.0),
    (0.25, 0.5, 0.0, 0.0),
    (0.2, 0.3, 0.5, 0.0),
)
implicit_table = (
    (0.0, 0.0, 0.0, 0.0),
    (0.25, 0.25, 0.0, 0.0),
    (0.25, 0.25, 0.25, 0.0),
    (0.15, 0.35, 0.25, 0.25),
)
section_weights = (0.15, 0.35, 0.25, 0.25)
implicit_diagonal = 0.25

MESH = pl.DeviceIdType.MESH
PAD = 8


GROUP = {"masks": 4, "diagonals": 2, "source": 2, "next": 2, "image": 2, "energy": 4, "rim": 4, "carry": 4, "both": 2, "gather": 2}
CHUNKS = 4


def grouped(name, low, high, value, store, carry):
    size = GROUP[name]

    def group(planes, carry):
        found = []
        for x in planes:
            carry, kept = value(x, carry)
            found.append(kept)
        for x, kept in zip(planes, found):
            store(x, kept)
        return carry

    turns = (high - low) // size
    carry = lax.fori_loop(
        0, turns, lambda t, c: group([low + t * size + k for k in range(size)], c), carry)
    rest = list(range(low + turns * size, high))
    return group(rest, carry) if rest else carry


def kernel(
    gx, gy, cot_hbm, speed_hbm, coeff_hbm, dirs_ref, out_ref,
    f0, f1, f2, f3, f4, f5, f6, fr0, fr1, fr2, fw0, fw1, fw2, dw0, dw1, dw2, base, cx, cy, cz, czm, px, py, pz, mx, my, mz, gdiag, fdiag,
    ysend, yrecv, landed, wpart, ypart, yside, corner_out, corner_in, slots,
    load_sem, send_sem, recv_sem, corner_send, corner_recv, sum_send, sum_recv,
):
    nx, ny, nz = out_ref.shape
    fields = (f0, f1, f2, f3, f4, f5, f6)
    fr, fw, dw = (fr0, fr1, fr2), (fw0, fw1, fw2), (dw0, dw1, dw2)
    me_x, me_y = lax.axis_index("gx"), lax.axis_index("gy")
    count = gx * gy
    me = me_x * gy + me_y
    own = pl.ds(PAD, ny)
    up = pl.ds(PAD + 1, ny)
    down = pl.ds(PAD - 1, ny)
    lane = lax.broadcasted_iota(jnp.int32, (ny, nz), 1)
    last_lane = lane == nz - 1
    low_x, low_y = me_x > 0, me_y > 0
    high_x, high_y = me_x < gx - 1, me_y < gy - 1

    def ahead_z(v):
        return pltpu.roll(v, nz - 1, 1)

    def behind_z(v):
        return pltpu.roll(v, 1, 1)

    chunks = CHUNKS if nx % CHUNKS == 0 else 1
    piece = nx // chunks

    def load(k, src, dst):
        copy = pltpu.make_async_copy(src, dst, load_sem.at[k])
        copy.start()
        return copy

    with jax.named_scope("loads"):
        cot_load = load(0, cot_hbm, fields[0].at[pl.ds(1, nx), own])
        loads = []
        for chunk in range(chunks):
            at = pl.ds(chunk * piece, piece)
            loads.append([
                load(1 + 6 * chunk + k, src, dst)
                for k, (src, dst) in enumerate((
                    (coeff_hbm.at[0, at], cx.at[pl.ds(1 + chunk * piece, piece)]),
                    (coeff_hbm.at[1, at], cy.at[at, own]),
                    (coeff_hbm.at[2, at], cz.at[at]),
                    (speed_hbm.at[0, at], px.at[at]),
                    (speed_hbm.at[1, at], py.at[at]),
                    (speed_hbm.at[2, at], pz.at[at]),
                ))
            ])

        plane = jnp.zeros((ny, nz), jnp.float32)
        for k in range(7):
            fields[k][0, own] = plane
            fields[k][nx + 1, own] = plane
        landed[0] = plane
        landed[1] = plane
        yrecv[...] = jnp.zeros_like(yrecv)
        corner_in[...] = jnp.zeros_like(corner_in)

        barrier = pltpu.get_barrier_semaphore()
        for off in range(1, count):
            to = {"gx": lax.rem(me_x + off // gy, gx), "gy": lax.rem(me_y + off % gy, gy)}
            pl.semaphore_signal(barrier, inc=1, device_id=to, device_id_type=MESH)

        cx[0] = plane
        mx[0] = plane

        def zero_rows(x, carry):
            cy[x, pl.ds(0, PAD)] = jnp.zeros((PAD, nz), jnp.float32)
            my[x, pl.ds(0, PAD)] = jnp.zeros((PAD, nz), jnp.float32)
            for k in range(1, 7):
                fields[k][x + 1, pl.ds(0, PAD)] = jnp.zeros((PAD, nz), jnp.float32)
                fields[k][x + 1, pl.ds(PAD + ny, PAD)] = jnp.zeros((PAD, nz), jnp.float32)
            return carry

        lax.fori_loop(0, nx, zero_rows, 0)

    def channel(tag, k, src, dst, axis, move):
        size, at = (gx, me_x) if axis == "gx" else (gy, me_y)
        return pltpu.make_async_remote_copy(
            src, dst, send_sem.at[tag, k], recv_sem.at[tag, k],
            device_id={axis: lax.rem(at + size + move, size)}, device_id_type=MESH)

    def x_down(tag, src, dst):
        return channel(tag, 0, src, dst, "gx", -1)

    def x_up(tag, src, dst):
        return channel(tag, 1, src, dst, "gx", 1)

    def y_down(tag, src):
        return channel(tag, 2, src, yrecv.at[tag, 1], "gy", -1)

    def y_up(tag):
        return channel(tag, 3, ysend.at[tag, 1], yrecv.at[tag, 0], "gy", 1)

    def copies(tag):
        field = fields[tag]
        partial = tag > 3
        return (
            x_down(tag, wpart.at[tag - 4] if partial else field.at[1, own], field.at[nx + 1, own]),
            x_up(tag, field.at[nx, own], field.at[0, own]),
            y_down(tag, ypart.at[tag - 4] if partial else ysend.at[tag, 0]),
            y_up(tag),
        )

    starts = (low_x, high_x, low_y, high_y)
    ends = (high_x, low_x, high_y, low_y)

    def start(tag, *which):
        every = copies(tag)
        for k in which:
            pl.when(starts[k])(every[k].start)

    def arrive(tag, *which):
        every = copies(tag)
        for k in which:
            pl.when(ends[k])(every[k].wait_recv)

    def sent(tag):
        for k, copy in enumerate(copies(tag)):
            pl.when(starts[k])(copy.wait_send)

    XD, XU, YD, YU = range(4)

    def corners(step):
        out = []
        for k, (rows, dx, dy) in enumerate(((pl.ds(0, 1), -1, 1), (pl.ds(1, 2), -1, -1), (pl.ds(3, 1), 1, -1))):
            to = {"gx": lax.rem(me_x + gx + dx, gx), "gy": lax.rem(me_y + gy + dy, gy)}
            copy = pltpu.make_async_remote_copy(
                corner_out.at[step, rows], corner_in.at[step, rows],
                corner_send.at[step, k], corner_recv.at[step, k], device_id=to, device_id_type=MESH)
            toward = [low_x if dx < 0 else high_x, low_y if dy < 0 else high_y]
            whence = [high_x if dx < 0 else low_x, high_y if dy < 0 else low_y]
            out.append((copy, jnp.logical_and(*toward), jnp.logical_and(*whence)))
        return out

    def unpack(tag):
        for x in range(nx):
            fields[tag][1 + x, pl.ds(PAD - 1, 1)] = yrecv[tag, 0, pl.ds(x, 1)]
            fields[tag][1 + x, pl.ds(PAD + ny, 1)] = yrecv[tag, 1, pl.ds(x, 1)]

    with jax.named_scope("barrier"):
        cot_load.wait()
        for x in range(nx):
            at = pl.ds(x, 1)
            ysend[0, 0, at] = fields[0][x + 1, pl.ds(PAD, 1)]
            ysend[0, 1, at] = fields[0][x + 1, pl.ds(PAD + ny - 1, 1)]
        dirs = [dirs_ref[d].astype(jnp.float32).T for d in range(3)]
        pl.semaphore_wait(barrier, count - 1)
    start(0, XD, XU, YD, YU)

    def upper(d, x):
        column = (lax.broadcasted_iota(jnp.int32, (nx, nz), 0) == x).astype(jnp.float32)
        return jnp.dot(dirs[d], column, preferred_element_type=jnp.float32) > 0.5

    def masks(x, carry):
        low = [jnp.where(upper(d, x), ref[x], 0.0) for d, ref in enumerate((px, py, pz))]
        return carry, (low, [ref[x] - m for m, ref in zip(low, (px, py, pz))], cz[x])

    def store_masks(x, kept):
        low, high, c = kept
        at = pl.ds(x, 1)
        mx[x + 1] = low[0]
        my[x, own] = low[1]
        mz[x] = jnp.where(last_lane, 0.0, low[2])
        px[x], py[x] = high[0], high[1]
        pz[x] = high[2]
        czm[x] = jnp.where(last_lane, 0.0, c)
        ysend[8, 1, at] = low[1][ny - 1:]
        ysend[7, 1, at] = cy[x, pl.ds(PAD + ny - 1, 1)]

    def diagonals(x, carry):
        p = pz[x]
        f = px[x] + mx[x] + py[x] + my[x, down] + p + behind_z(mz[x])
        g = cx[x + 1] + cx[x] + cy[x, own] + cy[x, down] + cz[x] + behind_z(czm[x])
        return carry, (f, g, jnp.where(last_lane, 0.0, p))

    def store_diagonals(x, kept):
        fdiag[x], gdiag[x], pz[x] = kept

    for chunk in range(chunks):
        low, high = chunk * piece, (chunk + 1) * piece
        with jax.named_scope("loadwait"):
            for copy in loads[chunk]:
                copy.wait()
        with jax.named_scope("masks"):
            grouped("masks", low, high, masks, store_masks, 0)
        with jax.named_scope("diagonals"):
            grouped("diagonals", low, high, diagonals, store_diagonals, 0)

    statics = (
        (x_up(7, cx.at[nx], landed.at[0]), y_up(7)),
        (x_up(8, mx.at[nx], landed.at[1]), y_up(8)),
    )
    for xu, yu in statics:
        pl.when(high_x)(xu.start)
        pl.when(high_y)(yu.start)

    def spread(ref, x):
        v = ref[x + 1, own]
        total = cx[x + 1] * ref[x + 2, own] + cx[x] * ref[x, own]
        total += cy[x, own] * ref[x + 1, up] + cy[x, down] * ref[x + 1, down]
        c = czm[x]
        total += c * ahead_z(v) + behind_z(c * v)
        return v, total - gdiag[x] * v

    def inner(ref, x):
        v = ref[x + 1, own]
        total = cx[1] * ref[2, own] if x == 0 else cx[x] * ref[x, own]
        total += cy[x, own] * ref[x + 1, up] + cy[x, down] * ref[x + 1, down]
        c = czm[x]
        total += c * ahead_z(v) + behind_z(c * v)
        return v - implicit_diagonal * (total - gdiag[x] * v)

    def carried(ref, x):
        v = ref[x + 1, own]
        total = px[x] * ref[x + 2, own] + mx[x] * ref[x, own]
        total += py[x] * ref[x + 1, up] + my[x, down] * ref[x + 1, down]
        total += pz[x] * ahead_z(v) + behind_z(mz[x] * v)
        return total - fdiag[x] * v

    def fold(v):
        return jnp.sum(v.reshape(v.shape[0] // 8, 8, nz), axis=0)

    nothing = jnp.zeros((8, nz), jnp.float32)

    def keep(tag, x, v):
        fields[tag][x + 1, own] = v
        ysend[tag, 0, pl.ds(x, 1)] = v[:1]
        ysend[tag, 1, pl.ds(x, 1)] = v[ny - 1:]

    row_x = lax.broadcasted_iota(jnp.int32, (nx, nz), 0)
    between = jnp.logical_and(row_x > 0, row_x < nx - 1)
    across_x = jnp.where(high_x, implicit_diagonal, 0.0)
    across_y = jnp.where(high_y, implicit_diagonal, 0.0)

    square = (lax.broadcasted_iota(jnp.int32, (8, nz), 0) == lax.broadcasted_iota(jnp.int32, (8, nz), 1))

    def send_sums(step, sums):
        rows = [jnp.sum(m, axis=0, keepdims=True) for m in sums]
        rows = jnp.concatenate(rows + [jnp.zeros((8 - len(rows), nz), jnp.float32)], axis=0)
        totals = jnp.broadcast_to(jnp.sum(rows, axis=1, keepdims=True), (8, nz))
        slots[step, me] = jnp.sum(jnp.where(square, totals, 0.0), axis=0, keepdims=True)
        for off in range(1, count):
            to = {"gx": lax.rem(me_x + off // gy, gx), "gy": lax.rem(me_y + off % gy, gy)}
            pltpu.make_async_remote_copy(
                slots.at[step, me], slots.at[step, me], sum_send.at[step], sum_recv.at[step],
                device_id=to, device_id_type=MESH).start()

    def all_sums(step):
        some = slots.at[step, pl.ds(0, count - 1)]
        return pltpu.make_async_remote_copy(
            some, some, sum_send.at[step], sum_recv.at[step],
            device_id={"gx": lax.rem(me_x + 1, gx)}, device_id_type=MESH)

    def read_sums(step):
        all_sums(step).wait_recv()
        total = jnp.broadcast_to(jnp.sum(slots[step], axis=0), (8, nz))
        total = jnp.sum(jnp.where(square, total, 0.0), axis=1, keepdims=True)
        total = jnp.broadcast_to(total, (8, nz))
        return [total[k:k + 1] for k in range(4)]

    weights = []
    for step, section in enumerate((3, 2, 1)):
        r_tag, w_tag = 1 + step, 4 + step
        r_ref, w_ref = fields[r_tag], fields[w_tag]

        def first_pass(x, m0):
            if step == 0:
                c_ref = fields[0]
                r, more = section_weights[3] * (spread(c_ref, x)[1] + carried(c_ref, x)), None
            else:
                r, more = following(x)
            return m0 + fold(r * r), (r, more)

        def store_first(x, kept):
            r, more = kept
            keep(r_tag, x, r)
            yside[5, pl.ds(x, 1)] = r[1:2]
            if more is not None:
                fr[step - 1][x], dw[step - 1][x] = more

        outer = (0, 1, nx - 1)
        m0 = nothing
        if step == 0:
            with jax.named_scope("arrive0"):
                arrive(0, XD, XU, YD, YU)
                unpack(0)
            with jax.named_scope("first"):
                m0 = grouped("source", 2, nx - 1, first_pass, store_first, m0)
            with jax.named_scope("statics"):
                for xu, yu in statics:
                    pl.when(low_x)(xu.wait_recv)
                    pl.when(low_y)(yu.wait_recv)
                cx[0] = landed[0]
                mx[0] = landed[1]
                gdiag[0] += cx[0]
                fdiag[0] += mx[0]
                head = pl.ds(0, 1)
                for x in range(nx):
                    at = pl.ds(x, 1)
                    row = yrecv[7, 0, at]
                    cy[x, pl.ds(PAD - 1, 1)] = row
                    g = gdiag[x, head] + row
                    gdiag[x, head] = g
                    yside[3, at] = g
                    row = yrecv[8, 0, at]
                    my[x, pl.ds(PAD - 1, 1)] = row
                    fdiag[x, head] += row
                    yside[0, at] = cx[x + 1, head] if x < nx - 1 else jnp.zeros((1, nz), jnp.float32)
                    yside[4, at] = cx[x, head] if x else jnp.zeros((1, nz), jnp.float32)
                    yside[1, at] = cy[x, pl.ds(PAD, 1)]
                    yside[2, at] = czm[x, head]
            with jax.named_scope("firstedge"):
                for x in outer:
                    m0, kept = first_pass(x, m0)
                    store_first(x, kept)
                start(r_tag, XD, XU)
                inside = jnp.logical_and(row_x > 1, row_x < nx - 1)
                change = section_weights[3] * (yrecv[7, 0] + yrecv[8, 0]) * (yrecv[0, 0] - ysend[0, 0])
                change = jnp.where(inside, change, 0.0)
                r = ysend[r_tag, 0]
                m0 += fold((2.0 * r + change) * change)
                ysend[r_tag, 0] = r + change
                for x in range(2, nx - 1):
                    r_ref[1 + x, pl.ds(PAD, 1)] = ysend[r_tag, 0, pl.ds(x, 1)]
        else:
            with jax.named_scope("firstedge"):
                for x in outer:
                    m0, kept = first_pass(x, m0)
                    store_first(x, kept)
                start(r_tag, XD, XU)
        with jax.named_scope("corners"):
            w0 = inner(r_ref, 0)
            wpart[step] = w0
            w1 = inner(r_ref, nx - 1)
            corner = r_ref[1, pl.ds(PAD, 1)]
            corner_out[step, 0] = cy[0, pl.ds(PAD + ny - 1, 1)] * r_ref[1, pl.ds(PAD + ny - 1, 1)]
            corner_out[step, 1] = cy[0, pl.ds(PAD - 1, 1)] * corner
            corner_out[step, 2] = cx[0, pl.ds(0, 1)] * corner
            corner_out[step, 3] = cx[nx, pl.ds(0, 1)] * r_ref[nx, pl.ds(PAD, 1)]
            start(w_tag, XD)
        if step:
            with jax.named_scope("first"):
                m0 = grouped("next", 2, nx - 1, first_pass, store_first, m0)
        with jax.named_scope("ysend"):
            start(r_tag, YD, YU)
            for copy, toward, _ in corners(step):
                pl.when(toward)(copy.start)
            v = ysend[r_tag, 0]
            c = yside[2]
            total = yside[0] * pltpu.roll(v, nx - 1, 0) + yside[4] * pltpu.roll(v, 1, 0)
            total += yside[1] * yside[5] + c * ahead_z(v) + behind_z(c * v)
            ypart[step] = v - implicit_diagonal * (total - yside[3] * v)
            start(w_tag, YD)

        def second_pass(x, sums):
            m1, m2 = sums
            r, d = spread(r_ref, x)
            w = r - implicit_diagonal * d
            return (m1 + fold(r * w), m2 + fold(w * w)), w

        def store_second(x, w):
            keep(w_tag, x, w)

        with jax.named_scope("image"):
            sums = grouped("image", 1, nx - 1, second_pass, store_second, (nothing, nothing))

        def energy(x, low, rows):
            at, above = pl.ds(PAD + low, rows), pl.ds(PAD + low + 1, rows)
            mid = pl.ds(low, rows)
            w = w_ref[x + 1, at]
            jump_x = w_ref[x + 2, at] - w
            jump_y = w_ref[x + 1, above] - w
            jump_z = jnp.where(last_lane[:rows], 0.0, ahead_z(w)) - w
            total = cx[x + 1, mid] * jump_x * jump_x + cy[x, at] * jump_y * jump_y
            return fold(total + cz[x, mid] * jump_z * jump_z)

        with jax.named_scope("energy"):
            m3 = grouped("energy", 1, nx - 2, lambda x, m: (m + energy(x, 8, ny - 16), None), lambda x, kept: None, nothing)

        with jax.named_scope("arrive_y"):
            arrive(r_tag, YD, YU)
        with jax.named_scope("yfix"):
            unpack(r_tag)
            m1, m2 = sums
            for side, face in ((0, yrecv[7, 0]), (1, ysend[7, 1])):
                change = jnp.where(between, -implicit_diagonal * face * yrecv[r_tag, side], 0.0)
                w = ysend[w_tag, side]
                ysend[w_tag, side] = w + change
                m1 += fold(ysend[r_tag, side] * change)
                m2 += fold((2.0 * w + change) * change)
            for x in range(1, nx - 1):
                w_ref[1 + x, pl.ds(PAD, 1)] = ysend[w_tag, 0, pl.ds(x, 1)]
                w_ref[1 + x, pl.ds(PAD + ny - 1, 1)] = ysend[w_tag, 1, pl.ds(x, 1)]
        with jax.named_scope("rim"):
            m3 = grouped(
                "rim", 1, nx - 2, lambda x, m: (m + energy(x, 0, 8) + energy(x, ny - 8, 8), None), lambda x, kept: None, m3)
        with jax.named_scope("arrive_x"):
            arrive(r_tag, XD, XU)
        with jax.named_scope("edges"):
            sums = (m1, m2)
            for x in (0, nx - 1):
                sums, w = second_pass(x, sums)
                store_second(x, w)
            m1, m2 = sums
            start(w_tag, XU, YU)
        with jax.named_scope("arrive_w"):
            arrive(w_tag, XD, YD)
            for copy, _, whence in corners(step):
                pl.when(whence)(copy.wait_recv)
        with jax.named_scope("close"):
            w_ref[nx + 1, own] = w_ref[nx + 1, own] - across_x * (cx[nx] * r_ref[nx, own])
            for k, y in ((0, 0), (1, ny - 1)):
                w_ref[nx + 1, pl.ds(PAD + y, 1)] -= implicit_diagonal * corner_in[step, k]
            above = yrecv[w_tag, 1] - across_y * (ysend[7, 1] * ysend[r_tag, 1])
            above -= jnp.where(row_x == 0, implicit_diagonal * corner_in[step, 3], 0.0)
            above -= jnp.where(row_x == nx - 1, implicit_diagonal * corner_in[step, 2], 0.0)
            yrecv[w_tag, 1] = above
            for x in (0, nx - 2, nx - 1):
                m3 += energy(x, 0, ny)
            m3 += fold(ysend[7, 1] * above * (above - 2.0 * ysend[w_tag, 1]))
            m3 = m2 + implicit_diagonal * m3
        with jax.named_scope("sendsums"):
            send_sums(step, (m0, m1, m2, m3))

        def store_r(x, kept):
            fr[step][x] = kept

        with jax.named_scope("carry"):
            grouped("carry", 0, nx, lambda x, c: (c, carried(r_ref, x)), store_r, 0)

        target = section - 1
        share = section_weights[target] / section_weights[3]

        def gather(x, carry):
            total = share * fields[1][x + 1, own]
            for k in range(step):
                total += explicit_table[3 - k][target] * fr[k][x] + implicit_table[3 - k][target] * dw[k][x]
            if target == 0:
                total += fields[0][x + 1, own]
                for k in range(step):
                    on_r, on_w = weights[k]
                    total += on_r * fields[1 + k][x + 1, own] + on_w * fields[4 + k][x + 1, own]
            return carry, total

        def store_base(x, kept):
            base[x] = kept

        with jax.named_scope("gather"):
            grouped("gather", 0, nx, gather, store_base, 0)

        with jax.named_scope("arrive_up"):
            arrive(w_tag, XU, YU)
            unpack(w_tag)

        def store_w(x, kept):
            fw[step][x], dw[step][x] = kept

        with jax.named_scope("both"):
            grouped("both", 0, nx, lambda x, c: (c, (carried(w_ref, x), spread(w_ref, x)[1])), store_w, 0)

        with jax.named_scope("allsums"):
            m0, m1, m2, m3 = read_sums(step)
        alpha = m0 / m1
        rr = alpha * alpha * m2 - m0
        ratio = rr / m0
        product = m1 - 2.0 * alpha * m2 + alpha * alpha * m3
        alpha_next = rr / (product - ratio * rr / alpha)
        on_r = alpha + alpha_next * (1.0 + ratio)
        on_w = -alpha_next * alpha
        weights.append((on_r, on_w))

        def following(x, step=step, section=section, target=target, on_r=on_r, on_w=on_w):
            r, w = fields[1 + step][x + 1, own], fields[4 + step][x + 1, own]
            advected = on_r * fr[step][x] + on_w * fw[step][x]
            diffused = (on_r / implicit_diagonal) * (r - w) + on_w * dw[step][x]
            total = base[x]
            total += explicit_table[section][target] * advected
            total += implicit_table[section][target] * diffused
            if target == 0:
                return total + on_r * r + on_w * w
            return total, (advected, diffused)

    def last(x, carry):
        out_ref[x] = following(x)
        return carry

    with jax.named_scope("last"):
        lax.fori_loop(0, nx, last, 0)
    with jax.named_scope("sends"):
        for xu, yu in statics:
            pl.when(high_x)(xu.wait_send)
            pl.when(high_y)(yu.wait_send)
        for tag in range(7):
            sent(tag)
        for step in range(3):
            for copy, toward, _ in corners(step):
                pl.when(toward)(copy.wait_send)
            all_sums(step).wait_send()


def local(gx, gy, cotangent, speed, coeff, dirs):
    nx, ny, nz = cotangent.shape
    f32 = jnp.float32
    rows = ny + 2 * PAD
    plain = pltpu.VMEM((nx, ny, nz), f32)
    dma = pltpu.SemaphoreType.DMA
    far = pl.BlockSpec(memory_space=pltpu.HBM)
    hbm = [pltpu.with_memory_space_constraint(v, pltpu.HBM) for v in (cotangent, speed, coeff)]
    return pl.pallas_call(
        functools.partial(kernel, gx, gy),
        out_shape=jax.ShapeDtypeStruct((nx, ny, nz), f32),
        in_specs=[far, far, far, pl.BlockSpec(memory_space=pltpu.VMEM)],
        out_specs=pl.BlockSpec(memory_space=pltpu.VMEM),
        scratch_shapes=[
            *[pltpu.VMEM((nx + 2, rows, nz), f32)] * 7,
            *[plain] * 9,
            plain,
            pltpu.VMEM((nx + 1, ny, nz), f32),
            pltpu.VMEM((nx, rows, nz), f32),
            plain, plain,
            plain, plain, plain,
            pltpu.VMEM((nx + 1, ny, nz), f32),
            pltpu.VMEM((nx, rows, nz), f32),
            plain,
            plain, plain,
            pltpu.VMEM((9, 2, nx, nz), f32),
            pltpu.VMEM((9, 2, nx, nz), f32),
            pltpu.VMEM((2, ny, nz), f32),
            pltpu.VMEM((3, ny, nz), f32),
            pltpu.VMEM((3, nx, nz), f32),
            pltpu.VMEM((6, nx, nz), f32),
            pltpu.VMEM((3, 4, 1, nz), f32),
            pltpu.VMEM((3, 4, 1, nz), f32),
            pltpu.VMEM((3, gx * gy, 1, nz), f32),
            dma((1 + 6 * CHUNKS,)), dma((9, 4)), dma((9, 4)),
            dma((3, 3)), dma((3, 3)), dma((3,)), dma((3,)),
        ],
        compiler_params=pltpu.CompilerParams(
            collective_id=0, has_side_effects=True, vmem_limit_bytes=46 * 1024 * 1024
        ),
    )(*hbm, dirs)


def solution(mesh):
    return jax.shard_map(
        functools.partial(local, mesh.shape["gx"], mesh.shape["gy"]),
        mesh=mesh,
        in_specs=(
            P("gx", "gy", None),
            P(None, "gx", "gy", None),
            P(None, "gx", "gy", None),
            P(None, "gx", "gy"),
        ),
        out_specs=P("gx", "gy", None),
        check_vma=False,
    )
```

```python
import functools

import jax
import jax.numpy as jnp
from jax import lax
from jax.experimental import pallas as pl
from jax.experimental.pallas import tpu as pltpu
from jax.sharding import PartitionSpec as P

explicit_table = (
    (0.0, 0.0, 0.0, 0.0),
    (0.5, 0.0, 0.0, 0.0),
    (0.25, 0.5, 0.0, 0.0),
    (0.2, 0.3, 0.5, 0.0),
)
implicit_table = (
    (0.0, 0.0, 0.0, 0.0),
    (0.25, 0.25, 0.0, 0.0),
    (0.25, 0.25, 0.25, 0.0),
    (0.15, 0.35, 0.25, 0.25),
)
section_weights = (0.15, 0.35, 0.25, 0.25)
implicit_diagonal = 0.25

MESH = pl.DeviceIdType.MESH
PAD = 8


GROUP = {"masks": 8, "diagonals": 8, "source": 15, "strip": 29, "next": 29, "image": 10, "energy": 14, "rim": 28, "carry": 16, "both": 8, "gather": 16, "last": 8}
CHUNKS = 4


def grouped(name, low, high, value, store, carry):
    size = GROUP[name]

    def group(planes, carry):
        found = []
        for x in planes:
            carry, kept = value(x, carry)
            found.append(kept)
        for x, kept in zip(planes, found):
            store(x, kept)
        return carry

    turns = (high - low) // size
    carry = lax.fori_loop(
        0, turns, lambda t, c: group([low + t * size + k for k in range(size)], c), carry)
    rest = list(range(low + turns * size, high))
    return group(rest, carry) if rest else carry


def kernel(
    gx, gy, cot_hbm, speed_hbm, coeff_hbm, dirs_hbm, out_ref,
    f0, f1, f2, f3, f4, f5, f6, fr0, fr1, fr2, fw0, fw1, fw2, dw0, dw1, dw2, base, cx, cy, cz, czm, px, py, pz, mx, my, mz, gdiag, fdiag,
    ysend, yrecv, dirs_ref, landed, wpart, ypart, yside, corner_out, corner_in, slots,
    load_sem, send_sem, recv_sem, corner_send, corner_recv, sum_send, sum_recv,
):
    nx, ny, nz = out_ref.shape
    fields = (f0, f1, f2, f3, f4, f5, f6)
    fr, fw, dw = (fr0, fr1, fr2), (fw0, fw1, fw2), (dw0, dw1, dw2)
    me_x, me_y = lax.axis_index("gx"), lax.axis_index("gy")
    count = gx * gy
    me = me_x * gy + me_y
    own = pl.ds(PAD, ny)
    up = pl.ds(PAD + 1, ny)
    down = pl.ds(PAD - 1, ny)
    lane = lax.broadcasted_iota(jnp.int32, (ny, nz), 1)
    last_lane = lane == nz - 1
    low_x, low_y = me_x > 0, me_y > 0
    high_x, high_y = me_x < gx - 1, me_y < gy - 1

    def ahead_z(v):
        return pltpu.roll(v, nz - 1, 1)

    def behind_z(v):
        return pltpu.roll(v, 1, 1)

    chunks = CHUNKS if nx % CHUNKS == 0 else 1
    piece = nx // chunks

    def load(k, src, dst):
        copy = pltpu.make_async_copy(src, dst, load_sem.at[k])
        copy.start()
        return copy

    with jax.named_scope("loads"):
        cot_load = load(0, cot_hbm, fields[0].at[pl.ds(1, nx), own])
        dirs_load = load(1 + 6 * chunks, dirs_hbm, dirs_ref)
        loads = []
        for chunk in range(chunks):
            at = pl.ds(chunk * piece, piece)
            loads.append([
                load(1 + 6 * chunk + k, src, dst)
                for k, (src, dst) in enumerate((
                    (coeff_hbm.at[0, at], cx.at[pl.ds(1 + chunk * piece, piece)]),
                    (coeff_hbm.at[1, at], cy.at[at, own]),
                    (coeff_hbm.at[2, at], cz.at[at]),
                    (speed_hbm.at[0, at], px.at[at]),
                    (speed_hbm.at[1, at], py.at[at]),
                    (speed_hbm.at[2, at], pz.at[at]),
                ))
            ])

        plane = jnp.zeros((ny, nz), jnp.float32)
        for k in range(7):
            fields[k][0, own] = plane
            fields[k][nx + 1, own] = plane
        landed[0] = plane
        landed[1] = plane
        yrecv[...] = jnp.zeros_like(yrecv)
        corner_in[...] = jnp.zeros_like(corner_in)

        barrier = pltpu.get_barrier_semaphore()
        for off in range(1, count):
            to = {"gx": lax.rem(me_x + off // gy, gx), "gy": lax.rem(me_y + off % gy, gy)}
            pl.semaphore_signal(barrier, inc=1, device_id=to, device_id_type=MESH)

        cx[0] = plane
        mx[0] = plane

        def zero_rows(x, carry):
            cy[x, pl.ds(0, PAD)] = jnp.zeros((PAD, nz), jnp.float32)
            my[x, pl.ds(0, PAD)] = jnp.zeros((PAD, nz), jnp.float32)
            for k in range(1, 7):
                fields[k][x + 1, pl.ds(0, PAD)] = jnp.zeros((PAD, nz), jnp.float32)
                fields[k][x + 1, pl.ds(PAD + ny, PAD)] = jnp.zeros((PAD, nz), jnp.float32)
            return carry

        lax.fori_loop(0, nx, zero_rows, 0)

    def channel(tag, k, src, dst, axis, move):
        size, at = (gx, me_x) if axis == "gx" else (gy, me_y)
        return pltpu.make_async_remote_copy(
            src, dst, send_sem.at[tag, k], recv_sem.at[tag, k],
            device_id={axis: lax.rem(at + size + move, size)}, device_id_type=MESH)

    def x_down(tag, src, dst):
        return channel(tag, 0, src, dst, "gx", -1)

    def x_up(tag, src, dst):
        return channel(tag, 1, src, dst, "gx", 1)

    def y_down(tag, src):
        return channel(tag, 2, src, yrecv.at[tag, 1], "gy", -1)

    def y_up(tag):
        return channel(tag, 3, ysend.at[tag, 1], yrecv.at[tag, 0], "gy", 1)

    def copies(tag):
        field = fields[tag]
        partial = tag > 3
        return (
            x_down(tag, wpart.at[tag - 4] if partial else field.at[1, own], field.at[nx + 1, own]),
            x_up(tag, field.at[nx, own], field.at[0, own]),
            y_down(tag, ypart.at[tag - 4] if partial else ysend.at[tag, 0]),
            y_up(tag),
        )

    starts = (low_x, high_x, low_y, high_y)
    ends = (high_x, low_x, high_y, low_y)

    def start(tag, *which):
        every = copies(tag)
        for k in which:
            pl.when(starts[k])(every[k].start)

    odd = lax.rem(me_x, 2) == 1

    def start_if(also, tag, k):
        pl.when(jnp.logical_and(also, starts[k]))(copies(tag)[k].start)

    def arrive(tag, *which):
        every = copies(tag)
        for k in which:
            pl.when(ends[k])(every[k].wait_recv)

    def sent(tag):
        for k, copy in enumerate(copies(tag)):
            pl.when(starts[k])(copy.wait_send)

    XD, XU, YD, YU = range(4)

    def corners(step):
        out = []
        for k, (rows, dx, dy) in enumerate(((pl.ds(0, 1), -1, 1), (pl.ds(1, 2), -1, -1), (pl.ds(3, 1), 1, -1))):
            to = {"gx": lax.rem(me_x + gx + dx, gx), "gy": lax.rem(me_y + gy + dy, gy)}
            copy = pltpu.make_async_remote_copy(
                corner_out.at[step, rows], corner_in.at[step, rows],
                corner_send.at[step, k], corner_recv.at[step, k], device_id=to, device_id_type=MESH)
            toward = [low_x if dx < 0 else high_x, low_y if dy < 0 else high_y]
            whence = [high_x if dx < 0 else low_x, high_y if dy < 0 else low_y]
            out.append((copy, jnp.logical_and(*toward), jnp.logical_and(*whence)))
        return out

    def unpack(tag):
        for x in range(nx):
            fields[tag][1 + x, pl.ds(PAD - 1, 1)] = yrecv[tag, 0, pl.ds(x, 1)]
            fields[tag][1 + x, pl.ds(PAD + ny, 1)] = yrecv[tag, 1, pl.ds(x, 1)]

    with jax.named_scope("barrier"):
        cot_load.wait()
        dirs_load.wait()
        for x in range(nx):
            at = pl.ds(x, 1)
            ysend[0, 0, at] = fields[0][x + 1, pl.ds(PAD, 1)]
            ysend[0, 1, at] = fields[0][x + 1, pl.ds(PAD + ny - 1, 1)]
        dirs = [dirs_ref[d].astype(jnp.float32).T for d in range(3)]
        pl.semaphore_wait(barrier, count - 1)
    start(0, XD, XU, YD, YU)

    def upper(d, x):
        column = (lax.broadcasted_iota(jnp.int32, (nx, nz), 0) == x).astype(jnp.float32)
        return jnp.dot(dirs[d], column, preferred_element_type=jnp.float32) > 0.5

    def masks(x, carry):
        low = [jnp.where(upper(d, x), ref[x], 0.0) for d, ref in enumerate((px, py, pz))]
        return carry, (low, [ref[x] - m for m, ref in zip(low, (px, py, pz))], cz[x])

    def store_masks(x, kept):
        low, high, c = kept
        at = pl.ds(x, 1)
        mx[x + 1] = low[0]
        my[x, own] = low[1]
        mz[x] = jnp.where(last_lane, 0.0, low[2])
        px[x], py[x] = high[0], high[1]
        pz[x] = high[2]
        czm[x] = jnp.where(last_lane, 0.0, c)
        ysend[8, 1, at] = low[1][ny - 1:]
        ysend[7, 1, at] = cy[x, pl.ds(PAD + ny - 1, 1)]

    def diagonals(x, carry):
        p = pz[x]
        f = px[x] + mx[x] + py[x] + my[x, down] + p + behind_z(mz[x])
        g = cx[x + 1] + cx[x] + cy[x, own] + cy[x, down] + cz[x] + behind_z(czm[x])
        return carry, (f, g, jnp.where(last_lane, 0.0, p))

    def store_diagonals(x, kept):
        fdiag[x], gdiag[x], pz[x] = kept

    for chunk in range(chunks):
        low, high = chunk * piece, (chunk + 1) * piece
        with jax.named_scope("loadwait"):
            for copy in loads[chunk]:
                copy.wait()
        with jax.named_scope("masks"):
            grouped("masks", low, high, masks, store_masks, 0)
        with jax.named_scope("diagonals"):
            grouped("diagonals", low, high, diagonals, store_diagonals, 0)

    statics = (
        (x_up(7, cx.at[nx], landed.at[0]), y_up(7)),
        (x_up(8, mx.at[nx], landed.at[1]), y_up(8)),
    )
    for xu, yu in statics:
        pl.when(high_x)(xu.start)
        pl.when(high_y)(yu.start)

    def spread(ref, x):
        v = ref[x + 1, own]
        total = cx[x + 1] * ref[x + 2, own] + cx[x] * ref[x, own]
        total += cy[x, own] * ref[x + 1, up] + cy[x, down] * ref[x + 1, down]
        c = czm[x]
        total += c * ahead_z(v) + behind_z(c * v)
        return v, total - gdiag[x] * v

    def inner(ref, x):
        v = ref[x + 1, own]
        total = cx[1] * ref[2, own] if x == 0 else cx[x] * ref[x, own]
        total += cy[x, own] * ref[x + 1, up] + cy[x, down] * ref[x + 1, down]
        c = czm[x]
        total += c * ahead_z(v) + behind_z(c * v)
        return v - implicit_diagonal * (total - gdiag[x] * v)

    def carried(ref, x):
        v = ref[x + 1, own]
        total = px[x] * ref[x + 2, own] + mx[x] * ref[x, own]
        total += py[x] * ref[x + 1, up] + my[x, down] * ref[x + 1, down]
        total += pz[x] * ahead_z(v) + behind_z(mz[x] * v)
        return total - fdiag[x] * v

    def fold(v):
        return jnp.sum(v.reshape(v.shape[0] // 8, 8, nz), axis=0)

    nothing = jnp.zeros((8, nz), jnp.float32)

    def keep(tag, x, v):
        fields[tag][x + 1, own] = v
        ysend[tag, 0, pl.ds(x, 1)] = v[:1]
        ysend[tag, 1, pl.ds(x, 1)] = v[ny - 1:]

    row_x = lax.broadcasted_iota(jnp.int32, (nx, nz), 0)
    between = jnp.logical_and(row_x > 0, row_x < nx - 1)
    across_x = jnp.where(high_x, implicit_diagonal, 0.0)
    across_y = jnp.where(high_y, implicit_diagonal, 0.0)

    square = (lax.broadcasted_iota(jnp.int32, (8, nz), 0) == lax.broadcasted_iota(jnp.int32, (8, nz), 1))

    def send_sums(step, sums):
        rows = [jnp.sum(m, axis=0, keepdims=True) for m in sums]
        rows = jnp.concatenate(rows + [jnp.zeros((8 - len(rows), nz), jnp.float32)], axis=0)
        totals = jnp.broadcast_to(jnp.sum(rows, axis=1, keepdims=True), (8, nz))
        slots[step, me] = jnp.sum(jnp.where(square, totals, 0.0), axis=0, keepdims=True)
        for off in range(1, count):
            to = {"gx": lax.rem(me_x + off // gy, gx), "gy": lax.rem(me_y + off % gy, gy)}
            pltpu.make_async_remote_copy(
                slots.at[step, me], slots.at[step, me], sum_send.at[step], sum_recv.at[step],
                device_id=to, device_id_type=MESH).start()

    def all_sums(step):
        some = slots.at[step, pl.ds(0, count - 1)]
        return pltpu.make_async_remote_copy(
            some, some, sum_send.at[step], sum_recv.at[step],
            device_id={"gx": lax.rem(me_x + 1, gx)}, device_id_type=MESH)

    def read_sums(step):
        all_sums(step).wait_recv()
        total = jnp.broadcast_to(jnp.sum(slots[step], axis=0), (8, nz))
        total = jnp.sum(jnp.where(square, total, 0.0), axis=1, keepdims=True)
        total = jnp.broadcast_to(total, (8, nz))
        return [total[k:k + 1] for k in range(4)]

    weights = []
    for step, section in enumerate((3, 2, 1)):
        r_tag, w_tag = 1 + step, 4 + step
        r_ref, w_ref = fields[r_tag], fields[w_tag]

        def first_pass(x, m0):
            if step == 0:
                c_ref = fields[0]
                r, more = section_weights[3] * (spread(c_ref, x)[1] + carried(c_ref, x)), None
            return m0 + fold(r * r), (r, more)

        def store_first(x, kept):
            r, more = kept
            keep(r_tag, x, r)
            yside[5, pl.ds(x, 1)] = r[1:2]

        def part(low, rows):
            at, mid = pl.ds(PAD + low, rows), pl.ds(low, rows)

            def value(x, m0):
                r, more = following(x, low, rows)
                return m0 + fold(r * r), (r, more)

            def store(x, kept):
                r, more = kept
                r_ref[x + 1, at] = r
                if low < 8:
                    ysend[r_tag, 0, pl.ds(x, 1)] = r[:1]
                    yside[5, pl.ds(x, 1)] = r[1:2]
                if low + rows == ny:
                    ysend[r_tag, 1, pl.ds(x, 1)] = r[rows - 1:]
                fr[step - 1][x, mid], dw[step - 1][x, mid] = more

            return value, store

        def send_x():
            corner = r_ref[1, pl.ds(PAD, 1)]
            corner_out[step, 0] = cy[0, pl.ds(PAD + ny - 1, 1)] * r_ref[1, pl.ds(PAD + ny - 1, 1)]
            corner_out[step, 1] = cy[0, pl.ds(PAD - 1, 1)] * corner
            corner_out[step, 2] = cx[0, pl.ds(0, 1)] * corner
            corner_out[step, 3] = cx[nx, pl.ds(0, 1)] * r_ref[nx, pl.ds(PAD, 1)]
            for copy, toward, _ in corners(step):
                pl.when(toward)(copy.start)
            start_if(True, r_tag, XD)
            start_if(odd, r_tag, XU)
            wpart[step] = inner(r_ref, 0)
            start_if(jnp.logical_not(odd), w_tag, XD)
            start_if(jnp.logical_not(odd), r_tag, XU)

        outer = (0, 1, nx - 1)
        m0 = nothing
        if step == 0:
            with jax.named_scope("arrive0"):
                arrive(0, XD, XU, YD, YU)
                unpack(0)
            with jax.named_scope("first"):
                m0 = grouped("source", 2, nx - 1, first_pass, store_first, m0)
            with jax.named_scope("statics"):
                for xu, yu in statics:
                    pl.when(low_x)(xu.wait_recv)
                    pl.when(low_y)(yu.wait_recv)
                cx[0] = landed[0]
                mx[0] = landed[1]
                gdiag[0] += cx[0]
                fdiag[0] += mx[0]
                head = pl.ds(0, 1)
                for x in range(nx):
                    at = pl.ds(x, 1)
                    row = yrecv[7, 0, at]
                    cy[x, pl.ds(PAD - 1, 1)] = row
                    g = gdiag[x, head] + row
                    gdiag[x, head] = g
                    yside[3, at] = g
                    row = yrecv[8, 0, at]
                    my[x, pl.ds(PAD - 1, 1)] = row
                    fdiag[x, head] += row
                    yside[0, at] = cx[x + 1, head] if x < nx - 1 else jnp.zeros((1, nz), jnp.float32)
                    yside[4, at] = cx[x, head] if x else jnp.zeros((1, nz), jnp.float32)
                    yside[1, at] = cy[x, pl.ds(PAD, 1)]
                    yside[2, at] = czm[x, head]
            with jax.named_scope("firstedge"):
                for x in outer:
                    m0, kept = first_pass(x, m0)
                    store_first(x, kept)
                inside = jnp.logical_and(row_x > 1, row_x < nx - 1)
                change = section_weights[3] * (yrecv[7, 0] + yrecv[8, 0]) * (yrecv[0, 0] - ysend[0, 0])
                change = jnp.where(inside, change, 0.0)
                r = ysend[r_tag, 0]
                m0 += fold((2.0 * r + change) * change)
                ysend[r_tag, 0] = r + change
                for x in range(2, nx - 1):
                    r_ref[1 + x, pl.ds(PAD, 1)] = ysend[r_tag, 0, pl.ds(x, 1)]
                send_x()
                start(r_tag, YD, YU)
        else:
            with jax.named_scope("firstedge"):
                value, store = part(0, ny)
                for x in outer:
                    m0, kept = value(x, m0)
                    store(x, kept)
                send_x()
            with jax.named_scope("strips"):
                for low in (0, ny - 8):
                    value, store = part(low, 8)
                    m0 = grouped("strip", 2, nx - 1, value, store, m0)
                start(r_tag, YD, YU)
        with jax.named_scope("corners"):
            v = ysend[r_tag, 0]
            c = yside[2]
            total = yside[0] * pltpu.roll(v, nx - 1, 0) + yside[4] * pltpu.roll(v, 1, 0)
            total += yside[1] * yside[5] + c * ahead_z(v) + behind_z(c * v)
            ypart[step] = v - implicit_diagonal * (total - yside[3] * v)
            start(w_tag, YD)
            start_if(odd, w_tag, XD)
        if step:
            value, store = part(8, ny - 16)
            with jax.named_scope("first"):
                m0 = grouped("next", 2, nx - 1, value, store, m0)

        def second_pass(x, sums):
            m1, m2 = sums
            r, d = spread(r_ref, x)
            w = r - implicit_diagonal * d
            return (m1 + fold(r * w), m2 + fold(w * w)), w

        def store_second(x, w):
            keep(w_tag, x, w)

        with jax.named_scope("image"):
            sums = grouped("image", 1, nx - 1, second_pass, store_second, (nothing, nothing))

        def energy(x, low, rows):
            at, above = pl.ds(PAD + low, rows), pl.ds(PAD + low + 1, rows)
            mid = pl.ds(low, rows)
            w = w_ref[x + 1, at]
            jump_x = w_ref[x + 2, at] - w
            jump_y = w_ref[x + 1, above] - w
            jump_z = jnp.where(last_lane[:rows], 0.0, ahead_z(w)) - w
            total = cx[x + 1, mid] * jump_x * jump_x + cy[x, at] * jump_y * jump_y
            return fold(total + cz[x, mid] * jump_z * jump_z)

        with jax.named_scope("energy"):
            m3 = grouped("energy", 1, nx - 2, lambda x, m: (m + energy(x, 8, ny - 16), None), lambda x, kept: None, nothing)

        with jax.named_scope("arrive_y"):
            arrive(r_tag, YD, YU)
        with jax.named_scope("yfix"):
            unpack(r_tag)
            m1, m2 = sums
            for side, face in ((0, yrecv[7, 0]), (1, ysend[7, 1])):
                change = jnp.where(between, -implicit_diagonal * face * yrecv[r_tag, side], 0.0)
                w = ysend[w_tag, side]
                ysend[w_tag, side] = w + change
                m1 += fold(ysend[r_tag, side] * change)
                m2 += fold((2.0 * w + change) * change)
            for x in range(1, nx - 1):
                w_ref[1 + x, pl.ds(PAD, 1)] = ysend[w_tag, 0, pl.ds(x, 1)]
                w_ref[1 + x, pl.ds(PAD + ny - 1, 1)] = ysend[w_tag, 1, pl.ds(x, 1)]
        with jax.named_scope("rim"):
            m3 = grouped(
                "rim", 1, nx - 2, lambda x, m: (m + energy(x, 0, 8) + energy(x, ny - 8, 8), None), lambda x, kept: None, m3)
        with jax.named_scope("arrive_x"):
            arrive(r_tag, XD, XU)
        with jax.named_scope("edges"):
            sums = (m1, m2)
            for x in (0, nx - 1):
                sums, w = second_pass(x, sums)
                store_second(x, w)
            m1, m2 = sums
        with jax.named_scope("arrive_w"):
            arrive(w_tag, XD, YD)
            for copy, _, whence in corners(step):
                pl.when(whence)(copy.wait_recv)
        with jax.named_scope("close"):
            w_ref[nx + 1, own] = w_ref[nx + 1, own] - across_x * (cx[nx] * r_ref[nx, own])
            for k, y in ((0, 0), (1, ny - 1)):
                w_ref[nx + 1, pl.ds(PAD + y, 1)] -= implicit_diagonal * corner_in[step, k]
            above = yrecv[w_tag, 1] - across_y * (ysend[7, 1] * ysend[r_tag, 1])
            above -= jnp.where(row_x == 0, implicit_diagonal * corner_in[step, 3], 0.0)
            above -= jnp.where(row_x == nx - 1, implicit_diagonal * corner_in[step, 2], 0.0)
            yrecv[w_tag, 1] = above
            for x in (0, nx - 2, nx - 1):
                m3 += energy(x, 0, ny)
            m3 += fold(ysend[7, 1] * above * (above - 2.0 * ysend[w_tag, 1]))
            m3 = m2 + implicit_diagonal * m3
        with jax.named_scope("sendsums"):
            send_sums(step, (m0, m1, m2, m3))
            start(w_tag, YU, XU)

        def store_r(x, kept):
            fr[step][x] = kept

        with jax.named_scope("carry"):
            grouped("carry", 0, nx, lambda x, c: (c, carried(r_ref, x)), store_r, 0)

        target = section - 1
        share = section_weights[target] / section_weights[3]

        def gather(x, carry):
            total = share * fields[1][x + 1, own]
            for k in range(step):
                total += explicit_table[3 - k][target] * fr[k][x] + implicit_table[3 - k][target] * dw[k][x]
            if target == 0:
                total += fields[0][x + 1, own]
                for k in range(step):
                    on_r, on_w = weights[k]
                    total += on_r * fields[1 + k][x + 1, own] + on_w * fields[4 + k][x + 1, own]
            return carry, total

        def store_base(x, kept):
            base[x] = kept

        with jax.named_scope("gather"):
            grouped("gather", 0, nx, gather, store_base, 0)

        with jax.named_scope("arrive_up"):
            arrive(w_tag, XU, YU)
            unpack(w_tag)

        def store_w(x, kept):
            fw[step][x], dw[step][x] = kept

        with jax.named_scope("both"):
            grouped("both", 0, nx, lambda x, c: (c, (carried(w_ref, x), spread(w_ref, x)[1])), store_w, 0)

        with jax.named_scope("allsums"):
            m0, m1, m2, m3 = read_sums(step)
        alpha = m0 / m1
        rr = alpha * alpha * m2 - m0
        ratio = rr / m0
        product = m1 - 2.0 * alpha * m2 + alpha * alpha * m3
        alpha_next = rr / (product - ratio * rr / alpha)
        on_r = alpha + alpha_next * (1.0 + ratio)
        on_w = -alpha_next * alpha
        weights.append((on_r, on_w))

        def following(x, low=0, rows=ny, step=step, section=section, target=target, on_r=on_r, on_w=on_w):
            at, mid = pl.ds(PAD + low, rows), pl.ds(low, rows)
            r, w = fields[1 + step][x + 1, at], fields[4 + step][x + 1, at]
            advected = on_r * fr[step][x, mid] + on_w * fw[step][x, mid]
            diffused = (on_r / implicit_diagonal) * (r - w) + on_w * dw[step][x, mid]
            total = base[x, mid]
            total += explicit_table[section][target] * advected
            total += implicit_table[section][target] * diffused
            if target == 0:
                return total + on_r * r + on_w * w
            return total, (advected, diffused)

    def store_out(x, kept):
        out_ref[x] = kept

    with jax.named_scope("last"):
        grouped("last", 0, nx, lambda x, c: (c, following(x)), store_out, 0)
    with jax.named_scope("sends"):
        for xu, yu in statics:
            pl.when(high_x)(xu.wait_send)
            pl.when(high_y)(yu.wait_send)
        for tag in range(7):
            sent(tag)
        for step in range(3):
            for copy, toward, _ in corners(step):
                pl.when(toward)(copy.wait_send)
            all_sums(step).wait_send()


def local(gx, gy, cotangent, speed, coeff, dirs):
    nx, ny, nz = cotangent.shape
    f32 = jnp.float32
    rows = ny + 2 * PAD
    plain = pltpu.VMEM((nx, ny, nz), f32)
    dma = pltpu.SemaphoreType.DMA
    far = pl.BlockSpec(memory_space=pltpu.HBM)
    hbm = [pltpu.with_memory_space_constraint(v, pltpu.HBM) for v in (cotangent, speed, coeff, dirs)]
    return pl.pallas_call(
        functools.partial(kernel, gx, gy),
        out_shape=jax.ShapeDtypeStruct((nx, ny, nz), f32),
        in_specs=[far] * 4,
        out_specs=pl.BlockSpec(memory_space=pltpu.VMEM),
        scratch_shapes=[
            *[pltpu.VMEM((nx + 2, rows, nz), f32)] * 7,
            *[plain] * 9,
            plain,
            pltpu.VMEM((nx + 1, ny, nz), f32),
            pltpu.VMEM((nx, rows, nz), f32),
            plain, plain,
            plain, plain, plain,
            pltpu.VMEM((nx + 1, ny, nz), f32),
            pltpu.VMEM((nx, rows, nz), f32),
            plain,
            plain, plain,
            pltpu.VMEM((9, 2, nx, nz), f32),
            pltpu.VMEM((9, 2, nx, nz), f32),
            pltpu.VMEM(dirs.shape, dirs.dtype),
            pltpu.VMEM((2, ny, nz), f32),
            pltpu.VMEM((3, ny, nz), f32),
            pltpu.VMEM((3, nx, nz), f32),
            pltpu.VMEM((6, nx, nz), f32),
            pltpu.VMEM((3, 4, 1, nz), f32),
            pltpu.VMEM((3, 4, 1, nz), f32),
            pltpu.VMEM((3, gx * gy, 1, nz), f32),
            dma((2 + 6 * CHUNKS,)), dma((9, 4)), dma((9, 4)),
            dma((3, 3)), dma((3, 3)), dma((3,)), dma((3,)),
        ],
        compiler_params=pltpu.CompilerParams(
            collective_id=0, has_side_effects=True, vmem_limit_bytes=46 * 1024 * 1024
        ),
    )(*hbm)


def solution(mesh):
    return jax.shard_map(
        functools.partial(local, mesh.shape["gx"], mesh.shape["gy"]),
        mesh=mesh,
        in_specs=(
            P("gx", "gy", None),
            P(None, "gx", "gy", None),
            P(None, "gx", "gy", None),
            P(None, "gx", "gy"),
        ),
        out_specs=P("gx", "gy", None),
        check_vma=False,
    )
```

```python
import functools

import jax
import jax.numpy as jnp
from jax import lax
from jax.experimental import pallas as pl
from jax.experimental.pallas import tpu as pltpu
from jax.sharding import PartitionSpec as P

explicit_table = (
    (0.0, 0.0, 0.0, 0.0),
    (0.5, 0.0, 0.0, 0.0),
    (0.25, 0.5, 0.0, 0.0),
    (0.2, 0.3, 0.5, 0.0),
)
implicit_table = (
    (0.0, 0.0, 0.0, 0.0),
    (0.25, 0.25, 0.0, 0.0),
    (0.25, 0.25, 0.25, 0.0),
    (0.15, 0.35, 0.25, 0.25),
)
section_weights = (0.15, 0.35, 0.25, 0.25)
implicit_diagonal = 0.25

MESH = pl.DeviceIdType.MESH
PAD = 8


GROUP = {"masks": 8, "diagonals": 8, "source": 15, "strip": 29, "next": 29, "image": 10, "energy": 14, "rim": 28, "carry": 16, "both": 8, "gather": 16, "last": 8}
CHUNKS = 4


def grouped(name, low, high, value, store, carry):
    size = GROUP[name]

    def group(planes, carry):
        found = []
        for x in planes:
            carry, kept = value(x, carry)
            found.append(kept)
        for x, kept in zip(planes, found):
            store(x, kept)
        return carry

    turns = (high - low) // size
    carry = lax.fori_loop(
        0, turns, lambda t, c: group([low + t * size + k for k in range(size)], c), carry)
    rest = list(range(low + turns * size, high))
    return group(rest, carry) if rest else carry


def kernel(
    gx, gy, cot_hbm, speed_hbm, coeff_hbm, dirs_hbm, out_base, out_r, out_w, out_scale,
    f0, f1, f2, f3, f4, f5, f6, fr0, fr1, fw0, fw1, dw0, dw1, base, cx, cy, cz, czm, px, py, pz, mx, my, mz, gdiag, fdiag,
    ysend, yrecv, dirs_ref, cx_top, mx_top, cy_top, py_top, landed, wpart, ypart, yside, corner_out, corner_in, slots,
    load_sem, send_sem, recv_sem, corner_send, corner_recv, sum_send, sum_recv,
):
    nx, ny, nz = out_base.shape
    fields = (f0, f1, f2, f3, f4, f5, f6)
    fr, fw, dw = (fr0, fr1), (fw0, fw1), (dw0, dw1)
    me_x, me_y = lax.axis_index("gx"), lax.axis_index("gy")
    count = gx * gy
    me = me_x * gy + me_y
    own = pl.ds(PAD, ny)
    up = pl.ds(PAD + 1, ny)
    down = pl.ds(PAD - 1, ny)
    lane = lax.broadcasted_iota(jnp.int32, (ny, nz), 1)
    last_lane = lane == nz - 1
    low_x, low_y = me_x > 0, me_y > 0
    high_x, high_y = me_x < gx - 1, me_y < gy - 1

    def ahead_z(v):
        return pltpu.roll(v, nz - 1, 1)

    def behind_z(v):
        return pltpu.roll(v, 1, 1)

    chunks = CHUNKS if nx % CHUNKS == 0 else 1
    piece = nx // chunks

    def load(k, src, dst):
        copy = pltpu.make_async_copy(src, dst, load_sem.at[k])
        copy.start()
        return copy

    with jax.named_scope("loads"):
        first = 2 + 6 * chunks
        tops = [
            load(first, coeff_hbm.at[0, nx - 1], cx_top),
            load(first + 1, speed_hbm.at[0, nx - 1], mx_top),
            load(first + 2, coeff_hbm.at[1, :, pl.ds(ny - 8, 8)], cy_top),
            load(first + 3, speed_hbm.at[1, :, pl.ds(ny - 8, 8)], py_top),
        ]
        cot_load = load(0, cot_hbm, fields[0].at[pl.ds(1, nx), own])
        dirs_load = load(1 + 6 * chunks, dirs_hbm, dirs_ref)
        loads = []
        for chunk in range(chunks):
            at = pl.ds(chunk * piece, piece)
            loads.append([
                load(1 + 6 * chunk + k, src, dst)
                for k, (src, dst) in enumerate((
                    (coeff_hbm.at[0, at], cx.at[pl.ds(1 + chunk * piece, piece)]),
                    (coeff_hbm.at[1, at], cy.at[at, own]),
                    (coeff_hbm.at[2, at], cz.at[at]),
                    (speed_hbm.at[0, at], px.at[at]),
                    (speed_hbm.at[1, at], py.at[at]),
                    (speed_hbm.at[2, at], pz.at[at]),
                ))
            ])

        plane = jnp.zeros((ny, nz), jnp.float32)
        for k in range(7):
            fields[k][0, own] = plane
            fields[k][nx + 1, own] = plane
        landed[0] = plane
        landed[1] = plane
        yrecv[...] = jnp.zeros_like(yrecv)
        corner_in[...] = jnp.zeros_like(corner_in)

        barrier = pltpu.get_barrier_semaphore()
        for off in range(1, count):
            to = {"gx": lax.rem(me_x + off // gy, gx), "gy": lax.rem(me_y + off % gy, gy)}
            pl.semaphore_signal(barrier, inc=1, device_id=to, device_id_type=MESH)

        cx[0] = plane
        mx[0] = plane

        def zero_rows(x, carry):
            cy[x, pl.ds(0, PAD)] = jnp.zeros((PAD, nz), jnp.float32)
            my[x, pl.ds(0, PAD)] = jnp.zeros((PAD, nz), jnp.float32)
            for k in range(7):
                fields[k][x + 1, pl.ds(0, PAD)] = jnp.zeros((PAD, nz), jnp.float32)
                fields[k][x + 1, pl.ds(PAD + ny, PAD)] = jnp.zeros((PAD, nz), jnp.float32)
            return carry

        lax.fori_loop(0, nx, zero_rows, 0)

    def channel(tag, k, src, dst, axis, move):
        size, at = (gx, me_x) if axis == "gx" else (gy, me_y)
        return pltpu.make_async_remote_copy(
            src, dst, send_sem.at[tag, k], recv_sem.at[tag, k],
            device_id={axis: lax.rem(at + size + move, size)}, device_id_type=MESH)

    def x_down(tag, src, dst):
        return channel(tag, 0, src, dst, "gx", -1)

    def x_up(tag, src, dst):
        return channel(tag, 1, src, dst, "gx", 1)

    def y_down(tag, src):
        return channel(tag, 2, src, yrecv.at[tag, 1], "gy", -1)

    def y_up(tag):
        return channel(tag, 3, ysend.at[tag, 1], yrecv.at[tag, 0], "gy", 1)

    def copies(tag):
        field = fields[tag]
        partial = tag > 3
        return (
            x_down(tag, wpart.at[tag - 4] if partial else field.at[1, own], field.at[nx + 1, own]),
            x_up(tag, field.at[nx, own], field.at[0, own]),
            y_down(tag, ypart.at[tag - 4] if partial else ysend.at[tag, 0]),
            y_up(tag),
        )

    starts = (low_x, high_x, low_y, high_y)
    ends = (high_x, low_x, high_y, low_y)

    def start(tag, *which):
        every = copies(tag)
        for k in which:
            pl.when(starts[k])(every[k].start)

    odd = lax.rem(me_x, 2) == 1

    def start_if(also, tag, k):
        pl.when(jnp.logical_and(also, starts[k]))(copies(tag)[k].start)

    def arrive(tag, *which):
        every = copies(tag)
        for k in which:
            pl.when(ends[k])(every[k].wait_recv)

    def sent(tag):
        for k, copy in enumerate(copies(tag)):
            pl.when(starts[k])(copy.wait_send)

    XD, XU, YD, YU = range(4)

    def corners(step):
        out = []
        for k, (rows, dx, dy) in enumerate(((pl.ds(0, 1), -1, 1), (pl.ds(1, 2), -1, -1), (pl.ds(3, 1), 1, -1))):
            to = {"gx": lax.rem(me_x + gx + dx, gx), "gy": lax.rem(me_y + gy + dy, gy)}
            copy = pltpu.make_async_remote_copy(
                corner_out.at[step, rows], corner_in.at[step, rows],
                corner_send.at[step, k], corner_recv.at[step, k], device_id=to, device_id_type=MESH)
            toward = [low_x if dx < 0 else high_x, low_y if dy < 0 else high_y]
            whence = [high_x if dx < 0 else low_x, high_y if dy < 0 else low_y]
            out.append((copy, jnp.logical_and(*toward), jnp.logical_and(*whence)))
        return out

    def unpack(tag):
        for x in range(nx):
            fields[tag][1 + x, pl.ds(PAD - 1, 1)] = yrecv[tag, 0, pl.ds(x, 1)]
            fields[tag][1 + x, pl.ds(PAD + ny, 1)] = yrecv[tag, 1, pl.ds(x, 1)]

    with jax.named_scope("barrier"):
        cot_load.wait()
        dirs_load.wait()
        for x in range(nx):
            at = pl.ds(x, 1)
            ysend[0, 0, at] = fields[0][x + 1, pl.ds(PAD, 1)]
            ysend[0, 1, at] = fields[0][x + 1, pl.ds(PAD + ny - 1, 1)]
        dirs = [dirs_ref[d].astype(jnp.float32).T for d in range(3)]

        def upper(d, x):
            column = (lax.broadcasted_iota(jnp.int32, (nx, nz), 0) == x).astype(jnp.float32)
            return jnp.dot(dirs[d], column, preferred_element_type=jnp.float32) > 0.5

        for copy in tops:
            copy.wait()
        mx_top[...] = jnp.where(upper(0, nx - 1), mx_top[...], 0.0)
        for x in range(nx):
            at = pl.ds(x, 1)
            ysend[7, 1, at] = cy_top[x, 7:]
            yside[6, at] = py_top[x, 7:]
        edge = jnp.broadcast_to(dirs_ref[1][:, ny - 1:], (nx, nz)) > 0
        ysend[8, 1] = jnp.where(edge, yside[6], 0.0)
        yside[6] = jnp.where(edge, 0.0, yside[6])
        pl.semaphore_wait(barrier, count - 1)
        start(0, YD, YU, XD, XU)
        statics = (
            (x_up(7, cx_top, landed.at[0]), y_up(7)),
            (x_up(8, mx_top, landed.at[1]), y_up(8)),
        )
        for xu, yu in statics:
            pl.when(high_x)(xu.start)
            pl.when(high_y)(yu.start)

    def masks(x, carry):
        low = [jnp.where(upper(d, x), ref[x], 0.0) for d, ref in enumerate((px, py, pz))]
        return carry, (low, [ref[x] - m for m, ref in zip(low, (px, py, pz))], cz[x])

    def store_masks(x, kept):
        low, high, c = kept
        mx[x + 1] = low[0]
        my[x, own] = low[1]
        mz[x] = jnp.where(last_lane, 0.0, low[2])
        px[x], py[x] = high[0], high[1]
        pz[x] = high[2]
        czm[x] = jnp.where(last_lane, 0.0, c)

    def diagonals(x, carry):
        p = pz[x]
        f = px[x] + mx[x] + py[x] + my[x, down] + p + behind_z(mz[x])
        g = cx[x + 1] + cx[x] + cy[x, own] + cy[x, down] + cz[x] + behind_z(czm[x])
        return carry, (f, g, jnp.where(last_lane, 0.0, p))

    def store_diagonals(x, kept):
        fdiag[x], gdiag[x], pz[x] = kept

    for chunk in range(chunks):
        low, high = chunk * piece, (chunk + 1) * piece
        with jax.named_scope("loadwait"):
            for copy in loads[chunk]:
                copy.wait()
        with jax.named_scope("masks"):
            grouped("masks", low, high, masks, store_masks, 0)
        with jax.named_scope("diagonals"):
            grouped("diagonals", low, high, diagonals, store_diagonals, 0)

    def spread(ref, x):
        v = ref[x + 1, own]
        total = cx[x + 1] * ref[x + 2, own] + cx[x] * ref[x, own]
        total += cy[x, own] * ref[x + 1, up] + cy[x, down] * ref[x + 1, down]
        c = czm[x]
        total += c * ahead_z(v) + behind_z(c * v)
        return v, total - gdiag[x] * v

    def inner(ref, x):
        v = ref[x + 1, own]
        total = cx[1] * ref[2, own] if x == 0 else cx[x] * ref[x, own]
        total += cy[x, own] * ref[x + 1, up] + cy[x, down] * ref[x + 1, down]
        c = czm[x]
        total += c * ahead_z(v) + behind_z(c * v)
        return v - implicit_diagonal * (total - gdiag[x] * v)

    def carried(ref, x):
        v = ref[x + 1, own]
        total = px[x] * ref[x + 2, own] + mx[x] * ref[x, own]
        total += py[x] * ref[x + 1, up] + my[x, down] * ref[x + 1, down]
        total += pz[x] * ahead_z(v) + behind_z(mz[x] * v)
        return total - fdiag[x] * v

    def fold(v):
        return jnp.sum(v.reshape(v.shape[0] // 8, 8, nz), axis=0)

    nothing = jnp.zeros((8, nz), jnp.float32)

    def keep(tag, x, v):
        fields[tag][x + 1, own] = v
        ysend[tag, 0, pl.ds(x, 1)] = v[:1]
        ysend[tag, 1, pl.ds(x, 1)] = v[ny - 1:]

    row_x = lax.broadcasted_iota(jnp.int32, (nx, nz), 0)
    between = jnp.logical_and(row_x > 0, row_x < nx - 1)
    across_x = jnp.where(high_x, implicit_diagonal, 0.0)
    across_y = jnp.where(high_y, implicit_diagonal, 0.0)

    square = (lax.broadcasted_iota(jnp.int32, (8, nz), 0) == lax.broadcasted_iota(jnp.int32, (8, nz), 1))

    def send_sums(step, sums):
        rows = [jnp.sum(m, axis=0, keepdims=True) for m in sums]
        rows = jnp.concatenate(rows + [jnp.zeros((8 - len(rows), nz), jnp.float32)], axis=0)
        totals = jnp.broadcast_to(jnp.sum(rows, axis=1, keepdims=True), (8, nz))
        slots[step, me] = jnp.sum(jnp.where(square, totals, 0.0), axis=0, keepdims=True)
        for off in range(1, count):
            to = {"gx": lax.rem(me_x + off // gy, gx), "gy": lax.rem(me_y + off % gy, gy)}
            pltpu.make_async_remote_copy(
                slots.at[step, me], slots.at[step, me], sum_send.at[step], sum_recv.at[step],
                device_id=to, device_id_type=MESH).start()

    def all_sums(step):
        some = slots.at[step, pl.ds(0, count - 1)]
        return pltpu.make_async_remote_copy(
            some, some, sum_send.at[step], sum_recv.at[step],
            device_id={"gx": lax.rem(me_x + 1, gx)}, device_id_type=MESH)

    def read_sums(step):
        all_sums(step).wait_recv()
        total = jnp.broadcast_to(jnp.sum(slots[step], axis=0), (8, nz))
        total = jnp.sum(jnp.where(square, total, 0.0), axis=1, keepdims=True)
        total = jnp.broadcast_to(total, (8, nz))
        return [total[k:k + 1] for k in range(4)]

    weights = []
    for step, section in enumerate((3, 2, 1)):
        r_tag, w_tag = 1 + step, 4 + step
        r_ref, w_ref = fields[r_tag], fields[w_tag]

        def first_pass(x, m0):
            if step == 0:
                c_ref = fields[0]
                r, more = section_weights[3] * (spread(c_ref, x)[1] + carried(c_ref, x)), None
            return m0 + fold(r * r), (r, more)

        def store_first(x, kept):
            r, more = kept
            keep(r_tag, x, r)
            yside[5, pl.ds(x, 1)] = r[1:2]

        def part(low, rows):
            at, mid = pl.ds(PAD + low, rows), pl.ds(low, rows)

            def value(x, m0):
                r, more = following(x, low, rows)
                return m0 + fold(r * r), (r, more)

            def store(x, kept):
                r, more = kept
                r_ref[x + 1, at] = r
                if low < 8:
                    ysend[r_tag, 0, pl.ds(x, 1)] = r[:1]
                    yside[5, pl.ds(x, 1)] = r[1:2]
                if low + rows == ny:
                    ysend[r_tag, 1, pl.ds(x, 1)] = r[rows - 1:]
                fr[step - 1][x, mid], dw[step - 1][x, mid] = more

            return value, store

        def send_x():
            corner = r_ref[1, pl.ds(PAD, 1)]
            corner_out[step, 0] = cy[0, pl.ds(PAD + ny - 1, 1)] * r_ref[1, pl.ds(PAD + ny - 1, 1)]
            corner_out[step, 1] = cy[0, pl.ds(PAD - 1, 1)] * corner
            corner_out[step, 2] = cx[0, pl.ds(0, 1)] * corner
            corner_out[step, 3] = cx[nx, pl.ds(0, 1)] * r_ref[nx, pl.ds(PAD, 1)]
            for copy, toward, _ in corners(step):
                pl.when(toward)(copy.start)
            start_if(True, r_tag, XD)
            start_if(odd, r_tag, XU)
            wpart[step] = inner(r_ref, 0)
            start_if(jnp.logical_not(odd), w_tag, XD)
            start_if(jnp.logical_not(odd), r_tag, XU)

        outer = (0, 1, nx - 1)
        m0 = nothing
        if step == 0:
            with jax.named_scope("first"):
                m0 = grouped("source", 2, nx - 1, first_pass, store_first, m0)
            with jax.named_scope("arrive0"):
                arrive(0, XD, XU, YD, YU)
                for x in outer:
                    fields[0][1 + x, pl.ds(PAD - 1, 1)] = yrecv[0, 0, pl.ds(x, 1)]
                    fields[0][1 + x, pl.ds(PAD + ny, 1)] = yrecv[0, 1, pl.ds(x, 1)]
            with jax.named_scope("statics"):
                for xu, yu in statics:
                    pl.when(low_x)(xu.wait_recv)
                    pl.when(low_y)(yu.wait_recv)
                cx[0] = landed[0]
                mx[0] = landed[1]
                gdiag[0] += cx[0]
                fdiag[0] += mx[0]
                head = pl.ds(0, 1)
                for x in range(nx):
                    at = pl.ds(x, 1)
                    row = yrecv[7, 0, at]
                    cy[x, pl.ds(PAD - 1, 1)] = row
                    g = gdiag[x, head] + row
                    gdiag[x, head] = g
                    yside[3, at] = g
                    row = yrecv[8, 0, at]
                    my[x, pl.ds(PAD - 1, 1)] = row
                    fdiag[x, head] += row
                    yside[0, at] = cx[x + 1, head] if x < nx - 1 else jnp.zeros((1, nz), jnp.float32)
                    yside[4, at] = cx[x, head] if x else jnp.zeros((1, nz), jnp.float32)
                    yside[1, at] = cy[x, pl.ds(PAD, 1)]
                    yside[2, at] = czm[x, head]
            with jax.named_scope("firstedge"):
                for x in outer:
                    m0, kept = first_pass(x, m0)
                    store_first(x, kept)
                send_x()
            with jax.named_scope("patch"):
                inside = jnp.logical_and(row_x > 1, row_x < nx - 1)
                for side, change in (
                    (0, (yrecv[7, 0] + yrecv[8, 0]) * (yrecv[0, 0] - ysend[0, 0])),
                    (1, (ysend[7, 1] + yside[6]) * yrecv[0, 1]),
                ):
                    change = jnp.where(inside, section_weights[3] * change, 0.0)
                    r = ysend[r_tag, side]
                    m0 += fold((2.0 * r + change) * change)
                    ysend[r_tag, side] = r + change
                for x in range(2, nx - 1):
                    r_ref[1 + x, pl.ds(PAD, 1)] = ysend[r_tag, 0, pl.ds(x, 1)]
                    r_ref[1 + x, pl.ds(PAD + ny - 1, 1)] = ysend[r_tag, 1, pl.ds(x, 1)]
                start(r_tag, YD, YU)
        else:
            with jax.named_scope("firstedge"):
                value, store = part(0, ny)
                for x in outer:
                    m0, kept = value(x, m0)
                    store(x, kept)
                send_x()
            with jax.named_scope("strips"):
                for low in (0, ny - 8):
                    value, store = part(low, 8)
                    m0 = grouped("strip", 2, nx - 1, value, store, m0)
                start(r_tag, YD, YU)
        with jax.named_scope("corners"):
            v = ysend[r_tag, 0]
            c = yside[2]
            total = yside[0] * pltpu.roll(v, nx - 1, 0) + yside[4] * pltpu.roll(v, 1, 0)
            total += yside[1] * yside[5] + c * ahead_z(v) + behind_z(c * v)
            ypart[step] = v - implicit_diagonal * (total - yside[3] * v)
            start(w_tag, YD)
            start_if(odd, w_tag, XD)
        if step:
            value, store = part(8, ny - 16)
            with jax.named_scope("first"):
                m0 = grouped("next", 2, nx - 1, value, store, m0)

        def second_pass(x, sums):
            m1, m2 = sums
            r, d = spread(r_ref, x)
            w = r - implicit_diagonal * d
            return (m1 + fold(r * w), m2 + fold(w * w)), w

        def store_second(x, w):
            keep(w_tag, x, w)

        with jax.named_scope("image"):
            sums = grouped("image", 1, nx - 1, second_pass, store_second, (nothing, nothing))

        def energy(x, low, rows):
            at, above = pl.ds(PAD + low, rows), pl.ds(PAD + low + 1, rows)
            mid = pl.ds(low, rows)
            w = w_ref[x + 1, at]
            jump_x = w_ref[x + 2, at] - w
            jump_y = w_ref[x + 1, above] - w
            jump_z = jnp.where(last_lane[:rows], 0.0, ahead_z(w)) - w
            total = cx[x + 1, mid] * jump_x * jump_x + cy[x, at] * jump_y * jump_y
            return fold(total + cz[x, mid] * jump_z * jump_z)

        with jax.named_scope("energy"):
            m3 = grouped("energy", 1, nx - 2, lambda x, m: (m + energy(x, 8, ny - 16), None), lambda x, kept: None, nothing)

        with jax.named_scope("arrive_y"):
            arrive(r_tag, YD, YU)
        with jax.named_scope("yfix"):
            unpack(r_tag)
            m1, m2 = sums
            for side, face in ((0, yrecv[7, 0]), (1, ysend[7, 1])):
                change = jnp.where(between, -implicit_diagonal * face * yrecv[r_tag, side], 0.0)
                w = ysend[w_tag, side]
                ysend[w_tag, side] = w + change
                m1 += fold(ysend[r_tag, side] * change)
                m2 += fold((2.0 * w + change) * change)
            for x in range(1, nx - 1):
                w_ref[1 + x, pl.ds(PAD, 1)] = ysend[w_tag, 0, pl.ds(x, 1)]
                w_ref[1 + x, pl.ds(PAD + ny - 1, 1)] = ysend[w_tag, 1, pl.ds(x, 1)]
        with jax.named_scope("rim"):
            m3 = grouped(
                "rim", 1, nx - 2, lambda x, m: (m + energy(x, 0, 8) + energy(x, ny - 8, 8), None), lambda x, kept: None, m3)
        with jax.named_scope("arrive_x"):
            arrive(r_tag, XD, XU)
        with jax.named_scope("edges"):
            sums = (m1, m2)
            for x in (0, nx - 1):
                sums, w = second_pass(x, sums)
                store_second(x, w)
            m1, m2 = sums
        with jax.named_scope("arrive_w"):
            arrive(w_tag, XD, YD)
            for copy, _, whence in corners(step):
                pl.when(whence)(copy.wait_recv)
        with jax.named_scope("close"):
            w_ref[nx + 1, own] = w_ref[nx + 1, own] - across_x * (cx[nx] * r_ref[nx, own])
            for k, y in ((0, 0), (1, ny - 1)):
                w_ref[nx + 1, pl.ds(PAD + y, 1)] -= implicit_diagonal * corner_in[step, k]
            above = yrecv[w_tag, 1] - across_y * (ysend[7, 1] * ysend[r_tag, 1])
            above -= jnp.where(row_x == 0, implicit_diagonal * corner_in[step, 3], 0.0)
            above -= jnp.where(row_x == nx - 1, implicit_diagonal * corner_in[step, 2], 0.0)
            for x in (0, nx - 2, nx - 1):
                m3 += energy(x, 0, ny)
            m3 += fold(ysend[7, 1] * above * (above - 2.0 * ysend[w_tag, 1]))
            m3 = m2 + implicit_diagonal * m3
        with jax.named_scope("sendsums"):
            send_sums(step, (m0, m1, m2, m3))
            start(w_tag, YU, XU)
            for x in range(nx):
                w_ref[1 + x, pl.ds(PAD + ny, 1)] = above[x:x + 1]

        target = section - 1
        final = target == 0
        on_f, on_d = explicit_table[section][target], implicit_table[section][target]

        def carry(x, c):
            f = carried(r_ref, x)
            if final:
                r = r_ref[x + 1, own]
                f = on_f * f + ((on_d / implicit_diagonal) * (r - w_ref[x + 1, own]) + r)
            return c, f

        def store_r(x, kept):
            (out_r if final else fr[step])[x] = kept

        with jax.named_scope("carry"):
            grouped("carry", 0, nx, carry, store_r, 0)

        share = section_weights[target] / section_weights[3]

        def gather(x, c):
            total = share * fields[1][x + 1, own]
            for k in range(step):
                total += explicit_table[3 - k][target] * fr[k][x] + implicit_table[3 - k][target] * dw[k][x]
            if target == 0:
                total += fields[0][x + 1, own]
                for k in range(step):
                    on_r, on_w = weights[k]
                    total += on_r * fields[1 + k][x + 1, own] + on_w * fields[4 + k][x + 1, own]
            return c, total

        def store_base(x, kept):
            (out_base if final else base)[x] = kept

        with jax.named_scope("gather"):
            grouped("gather", 0, nx, gather, store_base, 0)

        def store_w(x, kept):
            if final:
                out_w[x] = kept
            else:
                fw[step][x], dw[step][x] = kept

        def both(x, c):
            f, (w, d) = carried(w_ref, x), spread(w_ref, x)
            return c, on_f * f + on_d * d + w if final else (f, d)

        with jax.named_scope("both"):
            grouped("both", 1, nx, both, store_w, 0)
        with jax.named_scope("arrive_up"):
            arrive(w_tag, XU, YU)
        with jax.named_scope("late"):
            w_ref[1, pl.ds(PAD - 1, 1)] = yrecv[w_tag, 0, pl.ds(0, 1)]
            store_w(0, both(0, 0)[1])
            head = pl.ds(0, 1)
            owed_f = yrecv[8, 0] * yrecv[w_tag, 0]
            owed_d = yrecv[7, 0] * yrecv[w_tag, 0]
            owed = on_f * owed_f + on_d * owed_d
            for x in range(1, nx):
                if final:
                    out_w[x, head] += owed[x:x + 1]
                else:
                    fw[step][x, head] += owed_f[x:x + 1]
                    dw[step][x, head] += owed_d[x:x + 1]

        with jax.named_scope("allsums"):
            m0, m1, m2, m3 = read_sums(step)
        alpha = m0 / m1
        rr = alpha * alpha * m2 - m0
        ratio = rr / m0
        product = m1 - 2.0 * alpha * m2 + alpha * alpha * m3
        alpha_next = rr / (product - ratio * rr / alpha)
        on_r = alpha + alpha_next * (1.0 + ratio)
        on_w = -alpha_next * alpha
        weights.append((on_r, on_w))

        def following(x, low, rows, step=step, on_r=on_r, on_w=on_w, on_f=on_f, on_d=on_d):
            at, mid = pl.ds(PAD + low, rows), pl.ds(low, rows)
            r, w = fields[1 + step][x + 1, at], fields[4 + step][x + 1, at]
            advected = on_r * fr[step][x, mid] + on_w * fw[step][x, mid]
            diffused = (on_r / implicit_diagonal) * (r - w) + on_w * dw[step][x, mid]
            total = base[x, mid]
            total += on_f * advected + on_d * diffused
            return total, (advected, diffused)

    out_scale[...] = jnp.concatenate(weights[-1], axis=0)
    with jax.named_scope("sends"):
        for xu, yu in statics:
            pl.when(high_x)(xu.wait_send)
            pl.when(high_y)(yu.wait_send)
        for tag in range(7):
            sent(tag)
        for step in range(3):
            for copy, toward, _ in corners(step):
                pl.when(toward)(copy.wait_send)
            all_sums(step).wait_send()


def finish(base, on_r, on_w, scale, out_hbm, out, sem):
    nx = base.shape[0]
    chunks = CHUNKS if nx % CHUNKS == 0 else 1
    piece = nx // chunks
    copies = []
    for chunk in range(chunks):
        at = pl.ds(chunk * piece, piece)
        for x in range(chunk * piece, (chunk + 1) * piece):
            out[x] = base[x] + scale[:1] * on_r[x] + scale[1:] * on_w[x]
        copies.append(pltpu.make_async_copy(out.at[at], out_hbm.at[at], sem.at[chunk]))
        copies[-1].start()
    for copy in copies:
        copy.wait()


def local(gx, gy, cotangent, speed, coeff, dirs):
    nx, ny, nz = cotangent.shape
    f32 = jnp.float32
    rows = ny + 2 * PAD
    plain = pltpu.VMEM((nx, ny, nz), f32)
    dma = pltpu.SemaphoreType.DMA
    far = pl.BlockSpec(memory_space=pltpu.HBM)
    hbm = [pltpu.with_memory_space_constraint(v, pltpu.HBM) for v in (cotangent, speed, coeff, dirs)]
    whole = jax.ShapeDtypeStruct((nx, ny, nz), f32)
    total, on_r, on_w, scale = pl.pallas_call(
        functools.partial(kernel, gx, gy),
        out_shape=(whole, whole, whole, jax.ShapeDtypeStruct((2, nz), f32)),
        in_specs=[far] * 4,
        out_specs=(pl.BlockSpec(memory_space=pltpu.VMEM),) * 4,
        scratch_shapes=[
            *[pltpu.VMEM((nx + 2, rows, nz), f32)] * 7,
            *[plain] * 6,
            plain,
            pltpu.VMEM((nx + 1, ny, nz), f32),
            pltpu.VMEM((nx, rows, nz), f32),
            plain, plain,
            plain, plain, plain,
            pltpu.VMEM((nx + 1, ny, nz), f32),
            pltpu.VMEM((nx, rows, nz), f32),
            plain,
            plain, plain,
            pltpu.VMEM((9, 2, nx, nz), f32),
            pltpu.VMEM((9, 2, nx, nz), f32),
            pltpu.VMEM(dirs.shape, dirs.dtype),
            pltpu.VMEM((ny, nz), f32),
            pltpu.VMEM((ny, nz), f32),
            pltpu.VMEM((nx, 8, nz), f32),
            pltpu.VMEM((nx, 8, nz), f32),
            pltpu.VMEM((2, ny, nz), f32),
            pltpu.VMEM((3, ny, nz), f32),
            pltpu.VMEM((3, nx, nz), f32),
            pltpu.VMEM((7, nx, nz), f32),
            pltpu.VMEM((3, 4, 1, nz), f32),
            pltpu.VMEM((3, 4, 1, nz), f32),
            pltpu.VMEM((3, gx * gy, 1, nz), f32),
            dma((6 + 6 * CHUNKS,)), dma((9, 4)), dma((9, 4)),
            dma((3, 3)), dma((3, 3)), dma((3,)), dma((3,)),
        ],
        compiler_params=pltpu.CompilerParams(
            collective_id=0, has_side_effects=True, vmem_limit_bytes=46 * 1024 * 1024
        ),
    )(*hbm)
    return pl.pallas_call(
        finish,
        out_shape=whole,
        in_specs=[pl.BlockSpec(memory_space=pltpu.VMEM)] * 4,
        out_specs=pl.BlockSpec(memory_space=pltpu.HBM),
        scratch_shapes=[plain, dma((CHUNKS,))],
        compiler_params=pltpu.CompilerParams(vmem_limit_bytes=8 * 1024 * 1024),
    )(total, on_r, on_w, scale)


def solution(mesh):
    return jax.shard_map(
        functools.partial(local, mesh.shape["gx"], mesh.shape["gy"]),
        mesh=mesh,
        in_specs=(
            P("gx", "gy", None),
            P(None, "gx", "gy", None),
            P(None, "gx", "gy", None),
            P(None, "gx", "gy"),
        ),
        out_specs=P("gx", "gy", None),
        check_vma=False,
    )
```

```python
import functools

import jax
import jax.numpy as jnp
from jax import lax
from jax.experimental import pallas as pl
from jax.experimental.pallas import tpu as pltpu
from jax.sharding import PartitionSpec as P

explicit_table = (
    (0.0, 0.0, 0.0, 0.0),
    (0.5, 0.0, 0.0, 0.0),
    (0.25, 0.5, 0.0, 0.0),
    (0.2, 0.3, 0.5, 0.0),
)
implicit_table = (
    (0.0, 0.0, 0.0, 0.0),
    (0.25, 0.25, 0.0, 0.0),
    (0.25, 0.25, 0.25, 0.0),
    (0.15, 0.35, 0.25, 0.25),
)
section_weights = (0.15, 0.35, 0.25, 0.25)
implicit_diagonal = 0.25

MESH = pl.DeviceIdType.MESH
PAD = 8


GROUP = {"masks": 8, "diagonals": 8, "source": 15, "strip": 29, "next": 29, "image": 10, "energy": 14, "rim": 28, "carry": 16, "both": 8, "gather": 16, "last": 8}
CHUNKS = 4


def grouped(name, low, high, value, store, carry):
    size = GROUP[name]

    def group(planes, carry):
        found = []
        for x in planes:
            carry, kept = value(x, carry)
            found.append(kept)
        for x, kept in zip(planes, found):
            store(x, kept)
        return carry

    turns = (high - low) // size
    carry = lax.fori_loop(
        0, turns, lambda t, c: group([low + t * size + k for k in range(size)], c), carry)
    rest = list(range(low + turns * size, high))
    return group(rest, carry) if rest else carry


def kernel(
    gx, gy, cot_hbm, speed_hbm, coeff_hbm, dirs_hbm, out_base, out_r, out_w, out_scale,
    f0, f1, f2, f3, f4, f5, f6, fr0, fr1, fw0, fw1, dw0, dw1, base, cx, cy, cz, czm, px, py, pz, mx, my, mz, gdiag, fdiag,
    ysend, yrecv, dirs_ref, c_ends, cx_top, mx_top, cy_top, py_top, landed, wpart, ypart, yside, corner_out, corner_in, slots,
    load_sem, send_sem, recv_sem, corner_send, corner_recv, sum_send, sum_recv, known,
):
    nx, ny, nz = out_base.shape
    fields = (f0, f1, f2, f3, f4, f5, f6)
    fr, fw, dw = (fr0, fr1), (fw0, fw1), (dw0, dw1)
    me_x, me_y = lax.axis_index("gx"), lax.axis_index("gy")
    count = gx * gy
    me = me_x * gy + me_y
    own = pl.ds(PAD, ny)
    up = pl.ds(PAD + 1, ny)
    down = pl.ds(PAD - 1, ny)
    lane = lax.broadcasted_iota(jnp.int32, (ny, nz), 1)
    last_lane = lane == nz - 1
    low_x, low_y = me_x > 0, me_y > 0
    high_x, high_y = me_x < gx - 1, me_y < gy - 1

    def ahead_z(v):
        return pltpu.roll(v, nz - 1, 1)

    def behind_z(v):
        return pltpu.roll(v, 1, 1)

    chunks = CHUNKS if nx % CHUNKS == 0 else 1
    piece = nx // chunks

    def load(k, src, dst):
        copy = pltpu.make_async_copy(src, dst, load_sem.at[k])
        copy.start()
        return copy

    def greet(sem, d):
        for dx in (-d, 0, d):
            for dy in (-d, 0, d):
                if (dx, dy) == (0, 0) or abs(dx) >= gx or abs(dy) >= gy:
                    continue
                x, y = me_x + dx, me_y + dy
                there = jnp.logical_and(jnp.logical_and(x >= 0, x < gx), jnp.logical_and(y >= 0, y < gy))

                @pl.when(there)
                def _():
                    pl.semaphore_signal(sem, inc=1, device_id={"gx": x, "gy": y}, device_id_type=MESH)

    def greeted(sem, d):
        def near(at, size):
            return 1 + (at >= d).astype(jnp.int32) + (at + d < size).astype(jnp.int32)

        pl.semaphore_wait(sem, near(me_x, gx) * near(me_y, gy) - 1)

    reach = [1]
    while 2 * reach[-1] < max(gx, gy):
        reach.append(2 * reach[-1])

    def pass_on(k, last=False):
        while k < len(reach):
            greeted(known.at[k], reach[k])
            k += 1
            if k < len(reach):
                greet(known.at[k], reach[k])
            if not last:
                break

    with jax.named_scope("loads"):
        plane = jnp.zeros((ny, nz), jnp.float32)
        for k in range(7):
            fields[k][0, own] = plane
            fields[k][nx + 1, own] = plane
        landed[0] = plane
        landed[1] = plane
        yrecv[...] = jnp.zeros_like(yrecv)
        corner_in[...] = jnp.zeros_like(corner_in)

        barrier = pltpu.get_barrier_semaphore()
        greet(barrier, 1)

        first = 2 + 6 * chunks
        early = [
            load(first + 4, cot_hbm.at[0], c_ends.at[0]),
            load(first + 5, cot_hbm.at[nx - 1], c_ends.at[1]),
            load(1 + 6 * chunks, dirs_hbm, dirs_ref),
        ]
        tops = [
            load(first, coeff_hbm.at[0, nx - 1], cx_top),
            load(first + 1, speed_hbm.at[0, nx - 1], mx_top),
            load(first + 2, coeff_hbm.at[1, :, pl.ds(ny - 8, 8)], cy_top),
            load(first + 3, speed_hbm.at[1, :, pl.ds(ny - 8, 8)], py_top),
        ]
        cot_load = load(0, cot_hbm, fields[0].at[pl.ds(1, nx), own])
        loads = []
        for chunk in range(chunks):
            at = pl.ds(chunk * piece, piece)
            loads.append([
                load(1 + 6 * chunk + k, src, dst)
                for k, (src, dst) in enumerate((
                    (coeff_hbm.at[0, at], cx.at[pl.ds(1 + chunk * piece, piece)]),
                    (coeff_hbm.at[1, at], cy.at[at, own]),
                    (coeff_hbm.at[2, at], cz.at[at]),
                    (speed_hbm.at[0, at], px.at[at]),
                    (speed_hbm.at[1, at], py.at[at]),
                    (speed_hbm.at[2, at], pz.at[at]),
                ))
            ])

        cx[0] = plane
        mx[0] = plane

        def zero_rows(x, carry):
            cy[x, pl.ds(0, PAD)] = jnp.zeros((PAD, nz), jnp.float32)
            my[x, pl.ds(0, PAD)] = jnp.zeros((PAD, nz), jnp.float32)
            for k in range(7):
                fields[k][x + 1, pl.ds(0, PAD)] = jnp.zeros((PAD, nz), jnp.float32)
                fields[k][x + 1, pl.ds(PAD + ny, PAD)] = jnp.zeros((PAD, nz), jnp.float32)
            return carry

        lax.fori_loop(0, nx, zero_rows, 0)

    def channel(tag, k, src, dst, axis, move):
        size, at = (gx, me_x) if axis == "gx" else (gy, me_y)
        return pltpu.make_async_remote_copy(
            src, dst, send_sem.at[tag, k], recv_sem.at[tag, k],
            device_id={axis: lax.rem(at + size + move, size)}, device_id_type=MESH)

    def x_down(tag, src, dst):
        return channel(tag, 0, src, dst, "gx", -1)

    def x_up(tag, src, dst):
        return channel(tag, 1, src, dst, "gx", 1)

    def y_down(tag, src):
        return channel(tag, 2, src, yrecv.at[tag, 1], "gy", -1)

    def y_up(tag):
        return channel(tag, 3, ysend.at[tag, 1], yrecv.at[tag, 0], "gy", 1)

    def copies(tag):
        field = fields[tag]
        partial = tag > 3
        return (
            x_down(
                tag, wpart.at[tag - 4] if partial else field.at[1, own] if tag else c_ends.at[0], field.at[nx + 1, own]),
            x_up(tag, field.at[nx, own] if tag else c_ends.at[1], field.at[0, own]),
            y_down(tag, ypart.at[tag - 4] if partial else ysend.at[tag, 0]),
            y_up(tag),
        )

    starts = (low_x, high_x, low_y, high_y)
    ends = (high_x, low_x, high_y, low_y)

    def start(tag, *which):
        every = copies(tag)
        for k in which:
            pl.when(starts[k])(every[k].start)

    odd = lax.rem(me_x, 2) == 1

    def start_if(also, tag, k):
        pl.when(jnp.logical_and(also, starts[k]))(copies(tag)[k].start)

    def arrive(tag, *which):
        every = copies(tag)
        for k in which:
            pl.when(ends[k])(every[k].wait_recv)

    def sent(tag):
        for k, copy in enumerate(copies(tag)):
            pl.when(starts[k])(copy.wait_send)

    XD, XU, YD, YU = range(4)

    def corners(step):
        out = []
        for k, (rows, dx, dy) in enumerate(((pl.ds(0, 1), -1, 1), (pl.ds(1, 2), -1, -1), (pl.ds(3, 1), 1, -1))):
            to = {"gx": lax.rem(me_x + gx + dx, gx), "gy": lax.rem(me_y + gy + dy, gy)}
            copy = pltpu.make_async_remote_copy(
                corner_out.at[step, rows], corner_in.at[step, rows],
                corner_send.at[step, k], corner_recv.at[step, k], device_id=to, device_id_type=MESH)
            toward = [low_x if dx < 0 else high_x, low_y if dy < 0 else high_y]
            whence = [high_x if dx < 0 else low_x, high_y if dy < 0 else low_y]
            out.append((copy, jnp.logical_and(*toward), jnp.logical_and(*whence)))
        return out

    def unpack(tag):
        for x in range(nx):
            fields[tag][1 + x, pl.ds(PAD - 1, 1)] = yrecv[tag, 0, pl.ds(x, 1)]
            fields[tag][1 + x, pl.ds(PAD + ny, 1)] = yrecv[tag, 1, pl.ds(x, 1)]

    with jax.named_scope("barrier"):
        for copy in early + tops[:2]:
            copy.wait()
        dirs = [dirs_ref[d].astype(jnp.float32).T for d in range(3)]

        def upper(d, x):
            column = (lax.broadcasted_iota(jnp.int32, (nx, nz), 0) == x).astype(jnp.float32)
            return jnp.dot(dirs[d], column, preferred_element_type=jnp.float32) > 0.5

        mx_top[...] = jnp.where(upper(0, nx - 1), mx_top[...], 0.0)
        statics = (
            (x_up(7, cx_top, landed.at[0]), y_up(7)),
            (x_up(8, mx_top, landed.at[1]), y_up(8)),
        )
        greeted(barrier, 1)
        start(0, XD, XU)
        greet(known.at[0], reach[0])
        for xu, _ in statics:
            pl.when(high_x)(xu.start)
    with jax.named_scope("rows"):
        for copy in [cot_load] + tops[2:]:
            copy.wait()
        for x in range(nx):
            at = pl.ds(x, 1)
            ysend[0, 0, at] = fields[0][x + 1, pl.ds(PAD, 1)]
            ysend[0, 1, at] = fields[0][x + 1, pl.ds(PAD + ny - 1, 1)]
            ysend[7, 1, at] = cy_top[x, 7:]
            yside[6, at] = py_top[x, 7:]
        edge = jnp.broadcast_to(dirs_ref[1][:, ny - 1:], (nx, nz)) > 0
        ysend[8, 1] = jnp.where(edge, yside[6], 0.0)
        yside[6] = jnp.where(edge, 0.0, yside[6])
        start(0, YD, YU)
        for _, yu in statics:
            pl.when(high_y)(yu.start)

    def masks(x, carry):
        low = [jnp.where(upper(d, x), ref[x], 0.0) for d, ref in enumerate((px, py, pz))]
        return carry, (low, [ref[x] - m for m, ref in zip(low, (px, py, pz))], cz[x])

    def store_masks(x, kept):
        low, high, c = kept
        mx[x + 1] = low[0]
        my[x, own] = low[1]
        mz[x] = jnp.where(last_lane, 0.0, low[2])
        px[x], py[x] = high[0], high[1]
        pz[x] = high[2]
        czm[x] = jnp.where(last_lane, 0.0, c)

    def diagonals(x, carry):
        p = pz[x]
        f = px[x] + mx[x] + py[x] + my[x, down] + p + behind_z(mz[x])
        g = cx[x + 1] + cx[x] + cy[x, own] + cy[x, down] + cz[x] + behind_z(czm[x])
        return carry, (f, g, jnp.where(last_lane, 0.0, p))

    def store_diagonals(x, kept):
        fdiag[x], gdiag[x], pz[x] = kept

    for chunk in range(chunks):
        low, high = chunk * piece, (chunk + 1) * piece
        with jax.named_scope("loadwait"):
            for copy in loads[chunk]:
                copy.wait()
        with jax.named_scope("masks"):
            grouped("masks", low, high, masks, store_masks, 0)
        with jax.named_scope("diagonals"):
            grouped("diagonals", low, high, diagonals, store_diagonals, 0)

    pass_on(0)

    def spread(ref, x):
        v = ref[x + 1, own]
        total = cx[x + 1] * ref[x + 2, own] + cx[x] * ref[x, own]
        total += cy[x, own] * ref[x + 1, up] + cy[x, down] * ref[x + 1, down]
        c = czm[x]
        total += c * ahead_z(v) + behind_z(c * v)
        return v, total - gdiag[x] * v

    def inner(ref, x):
        v = ref[x + 1, own]
        total = cx[1] * ref[2, own] if x == 0 else cx[x] * ref[x, own]
        total += cy[x, own] * ref[x + 1, up] + cy[x, down] * ref[x + 1, down]
        c = czm[x]
        total += c * ahead_z(v) + behind_z(c * v)
        return v - implicit_diagonal * (total - gdiag[x] * v)

    def carried(ref, x):
        v = ref[x + 1, own]
        total = px[x] * ref[x + 2, own] + mx[x] * ref[x, own]
        total += py[x] * ref[x + 1, up] + my[x, down] * ref[x + 1, down]
        total += pz[x] * ahead_z(v) + behind_z(mz[x] * v)
        return total - fdiag[x] * v

    def fold(v):
        return jnp.sum(v.reshape(v.shape[0] // 8, 8, nz), axis=0)

    nothing = jnp.zeros((8, nz), jnp.float32)

    def keep(tag, x, v):
        fields[tag][x + 1, own] = v
        ysend[tag, 0, pl.ds(x, 1)] = v[:1]
        ysend[tag, 1, pl.ds(x, 1)] = v[ny - 1:]

    row_x = lax.broadcasted_iota(jnp.int32, (nx, nz), 0)
    between = jnp.logical_and(row_x > 0, row_x < nx - 1)
    across_x = jnp.where(high_x, implicit_diagonal, 0.0)
    across_y = jnp.where(high_y, implicit_diagonal, 0.0)

    square = (lax.broadcasted_iota(jnp.int32, (8, nz), 0) == lax.broadcasted_iota(jnp.int32, (8, nz), 1))

    def send_sums(step, sums):
        rows = [jnp.sum(m, axis=0, keepdims=True) for m in sums]
        rows = jnp.concatenate(rows + [jnp.zeros((8 - len(rows), nz), jnp.float32)], axis=0)
        totals = jnp.broadcast_to(jnp.sum(rows, axis=1, keepdims=True), (8, nz))
        slots[step, me] = jnp.sum(jnp.where(square, totals, 0.0), axis=0, keepdims=True)
        for off in range(1, count):
            to = {"gx": lax.rem(me_x + off // gy, gx), "gy": lax.rem(me_y + off % gy, gy)}
            pltpu.make_async_remote_copy(
                slots.at[step, me], slots.at[step, me], sum_send.at[step], sum_recv.at[step],
                device_id=to, device_id_type=MESH).start()

    def all_sums(step):
        some = slots.at[step, pl.ds(0, count - 1)]
        return pltpu.make_async_remote_copy(
            some, some, sum_send.at[step], sum_recv.at[step],
            device_id={"gx": lax.rem(me_x + 1, gx)}, device_id_type=MESH)

    def read_sums(step):
        all_sums(step).wait_recv()
        total = jnp.broadcast_to(jnp.sum(slots[step], axis=0), (8, nz))
        total = jnp.sum(jnp.where(square, total, 0.0), axis=1, keepdims=True)
        total = jnp.broadcast_to(total, (8, nz))
        return [total[k:k + 1] for k in range(4)]

    weights = []
    for step, section in enumerate((3, 2, 1)):
        r_tag, w_tag = 1 + step, 4 + step
        r_ref, w_ref = fields[r_tag], fields[w_tag]

        def first_pass(x, m0):
            if step == 0:
                c_ref = fields[0]
                r, more = section_weights[3] * (spread(c_ref, x)[1] + carried(c_ref, x)), None
            return m0 + fold(r * r), (r, more)

        def store_first(x, kept):
            r, more = kept
            keep(r_tag, x, r)
            yside[5, pl.ds(x, 1)] = r[1:2]

        def part(low, rows):
            at, mid = pl.ds(PAD + low, rows), pl.ds(low, rows)

            def value(x, m0):
                r, more = following(x, low, rows)
                return m0 + fold(r * r), (r, more)

            def store(x, kept):
                r, more = kept
                r_ref[x + 1, at] = r
                if low < 8:
                    ysend[r_tag, 0, pl.ds(x, 1)] = r[:1]
                    yside[5, pl.ds(x, 1)] = r[1:2]
                if low + rows == ny:
                    ysend[r_tag, 1, pl.ds(x, 1)] = r[rows - 1:]
                fr[step - 1][x, mid], dw[step - 1][x, mid] = more

            return value, store

        def send_x():
            corner = r_ref[1, pl.ds(PAD, 1)]
            corner_out[step, 0] = cy[0, pl.ds(PAD + ny - 1, 1)] * r_ref[1, pl.ds(PAD + ny - 1, 1)]
            corner_out[step, 1] = cy[0, pl.ds(PAD - 1, 1)] * corner
            corner_out[step, 2] = cx[0, pl.ds(0, 1)] * corner
            corner_out[step, 3] = cx[nx, pl.ds(0, 1)] * r_ref[nx, pl.ds(PAD, 1)]
            for copy, toward, _ in corners(step):
                pl.when(toward)(copy.start)
            start_if(True, r_tag, XD)
            start_if(odd, r_tag, XU)
            wpart[step] = inner(r_ref, 0)
            start_if(jnp.logical_not(odd), w_tag, XD)
            start_if(jnp.logical_not(odd), r_tag, XU)

        outer = (0, 1, nx - 1)
        m0 = nothing
        if step == 0:
            with jax.named_scope("first"):
                m0 = grouped("source", 2, nx - 1, first_pass, store_first, m0)
            with jax.named_scope("arrive0"):
                arrive(0, XD, XU, YD, YU)
                for x in outer:
                    fields[0][1 + x, pl.ds(PAD - 1, 1)] = yrecv[0, 0, pl.ds(x, 1)]
                    fields[0][1 + x, pl.ds(PAD + ny, 1)] = yrecv[0, 1, pl.ds(x, 1)]
            with jax.named_scope("statics"):
                for xu, yu in statics:
                    pl.when(low_x)(xu.wait_recv)
                    pl.when(low_y)(yu.wait_recv)
                cx[0] = landed[0]
                mx[0] = landed[1]
                gdiag[0] += cx[0]
                fdiag[0] += mx[0]
                head = pl.ds(0, 1)
                for x in range(nx):
                    at = pl.ds(x, 1)
                    row = yrecv[7, 0, at]
                    cy[x, pl.ds(PAD - 1, 1)] = row
                    g = gdiag[x, head] + row
                    gdiag[x, head] = g
                    yside[3, at] = g
                    row = yrecv[8, 0, at]
                    my[x, pl.ds(PAD - 1, 1)] = row
                    fdiag[x, head] += row
                    yside[0, at] = cx[x + 1, head] if x < nx - 1 else jnp.zeros((1, nz), jnp.float32)
                    yside[4, at] = cx[x, head] if x else jnp.zeros((1, nz), jnp.float32)
                    yside[1, at] = cy[x, pl.ds(PAD, 1)]
                    yside[2, at] = czm[x, head]
            with jax.named_scope("firstedge"):
                for x in outer:
                    m0, kept = first_pass(x, m0)
                    store_first(x, kept)
                send_x()
            with jax.named_scope("patch"):
                inside = jnp.logical_and(row_x > 1, row_x < nx - 1)
                for side, change in (
                    (0, (yrecv[7, 0] + yrecv[8, 0]) * (yrecv[0, 0] - ysend[0, 0])),
                    (1, (ysend[7, 1] + yside[6]) * yrecv[0, 1]),
                ):
                    change = jnp.where(inside, section_weights[3] * change, 0.0)
                    r = ysend[r_tag, side]
                    m0 += fold((2.0 * r + change) * change)
                    ysend[r_tag, side] = r + change
                for x in range(2, nx - 1):
                    r_ref[1 + x, pl.ds(PAD, 1)] = ysend[r_tag, 0, pl.ds(x, 1)]
                    r_ref[1 + x, pl.ds(PAD + ny - 1, 1)] = ysend[r_tag, 1, pl.ds(x, 1)]
                start(r_tag, YD, YU)
        else:
            with jax.named_scope("firstedge"):
                value, store = part(0, ny)
                for x in outer:
                    m0, kept = value(x, m0)
                    store(x, kept)
                send_x()
            with jax.named_scope("strips"):
                for low in (0, ny - 8):
                    value, store = part(low, 8)
                    m0 = grouped("strip", 2, nx - 1, value, store, m0)
                start(r_tag, YD, YU)
        with jax.named_scope("corners"):
            v = ysend[r_tag, 0]
            c = yside[2]
            total = yside[0] * pltpu.roll(v, nx - 1, 0) + yside[4] * pltpu.roll(v, 1, 0)
            total += yside[1] * yside[5] + c * ahead_z(v) + behind_z(c * v)
            ypart[step] = v - implicit_diagonal * (total - yside[3] * v)
            start(w_tag, YD)
            start_if(odd, w_tag, XD)
        if step:
            value, store = part(8, ny - 16)
            with jax.named_scope("first"):
                m0 = grouped("next", 2, nx - 1, value, store, m0)

        def second_pass(x, sums):
            m1, m2 = sums
            r, d = spread(r_ref, x)
            w = r - implicit_diagonal * d
            return (m1 + fold(r * w), m2 + fold(w * w)), w

        def store_second(x, w):
            keep(w_tag, x, w)

        if step == 0:
            pass_on(1)
        with jax.named_scope("image"):
            sums = grouped("image", 1, nx - 1, second_pass, store_second, (nothing, nothing))

        def energy(x, low, rows):
            at, above = pl.ds(PAD + low, rows), pl.ds(PAD + low + 1, rows)
            mid = pl.ds(low, rows)
            w = w_ref[x + 1, at]
            jump_x = w_ref[x + 2, at] - w
            jump_y = w_ref[x + 1, above] - w
            jump_z = jnp.where(last_lane[:rows], 0.0, ahead_z(w)) - w
            total = cx[x + 1, mid] * jump_x * jump_x + cy[x, at] * jump_y * jump_y
            return fold(total + cz[x, mid] * jump_z * jump_z)

        with jax.named_scope("energy"):
            m3 = grouped("energy", 1, nx - 2, lambda x, m: (m + energy(x, 8, ny - 16), None), lambda x, kept: None, nothing)

        with jax.named_scope("arrive_y"):
            arrive(r_tag, YD, YU)
        with jax.named_scope("yfix"):
            unpack(r_tag)
            m1, m2 = sums
            for side, face in ((0, yrecv[7, 0]), (1, ysend[7, 1])):
                change = jnp.where(between, -implicit_diagonal * face * yrecv[r_tag, side], 0.0)
                w = ysend[w_tag, side]
                ysend[w_tag, side] = w + change
                m1 += fold(ysend[r_tag, side] * change)
                m2 += fold((2.0 * w + change) * change)
            for x in range(1, nx - 1):
                w_ref[1 + x, pl.ds(PAD, 1)] = ysend[w_tag, 0, pl.ds(x, 1)]
                w_ref[1 + x, pl.ds(PAD + ny - 1, 1)] = ysend[w_tag, 1, pl.ds(x, 1)]
        with jax.named_scope("rim"):
            m3 = grouped(
                "rim", 1, nx - 2, lambda x, m: (m + energy(x, 0, 8) + energy(x, ny - 8, 8), None), lambda x, kept: None, m3)
        with jax.named_scope("arrive_x"):
            arrive(r_tag, XD, XU)
        with jax.named_scope("edges"):
            sums = (m1, m2)
            for x in (0, nx - 1):
                sums, w = second_pass(x, sums)
                store_second(x, w)
            m1, m2 = sums
        with jax.named_scope("arrive_w"):
            arrive(w_tag, XD, YD)
            for copy, _, whence in corners(step):
                pl.when(whence)(copy.wait_recv)
        with jax.named_scope("close"):
            w_ref[nx + 1, own] = w_ref[nx + 1, own] - across_x * (cx[nx] * r_ref[nx, own])
            for k, y in ((0, 0), (1, ny - 1)):
                w_ref[nx + 1, pl.ds(PAD + y, 1)] -= implicit_diagonal * corner_in[step, k]
            above = yrecv[w_tag, 1] - across_y * (ysend[7, 1] * ysend[r_tag, 1])
            above -= jnp.where(row_x == 0, implicit_diagonal * corner_in[step, 3], 0.0)
            above -= jnp.where(row_x == nx - 1, implicit_diagonal * corner_in[step, 2], 0.0)
            for x in (0, nx - 2, nx - 1):
                m3 += energy(x, 0, ny)
            m3 += fold(ysend[7, 1] * above * (above - 2.0 * ysend[w_tag, 1]))
            m3 = m2 + implicit_diagonal * m3
        with jax.named_scope("sendsums"):
            if step == 0:
                pass_on(2, last=True)
            send_sums(step, (m0, m1, m2, m3))
            start(w_tag, YU, XU)
            for x in range(nx):
                w_ref[1 + x, pl.ds(PAD + ny, 1)] = above[x:x + 1]

        target = section - 1
        final = target == 0
        on_f, on_d = explicit_table[section][target], implicit_table[section][target]

        def carry(x, c):
            f = carried(r_ref, x)
            if final:
                r = r_ref[x + 1, own]
                f = on_f * f + ((on_d / implicit_diagonal) * (r - w_ref[x + 1, own]) + r)
            return c, f

        def store_r(x, kept):
            (out_r if final else fr[step])[x] = kept

        with jax.named_scope("carry"):
            grouped("carry", 0, nx, carry, store_r, 0)

        share = section_weights[target] / section_weights[3]

        def gather(x, c):
            total = share * fields[1][x + 1, own]
            for k in range(step):
                total += explicit_table[3 - k][target] * fr[k][x] + implicit_table[3 - k][target] * dw[k][x]
            if target == 0:
                total += fields[0][x + 1, own]
                for k in range(step):
                    on_r, on_w = weights[k]
                    total += on_r * fields[1 + k][x + 1, own] + on_w * fields[4 + k][x + 1, own]
            return c, total

        def store_base(x, kept):
            (out_base if final else base)[x] = kept

        with jax.named_scope("gather"):
            grouped("gather", 0, nx, gather, store_base, 0)

        def store_w(x, kept):
            if final:
                out_w[x] = kept
            else:
                fw[step][x], dw[step][x] = kept

        def both(x, c):
            f, (w, d) = carried(w_ref, x), spread(w_ref, x)
            return c, on_f * f + on_d * d + w if final else (f, d)

        with jax.named_scope("both"):
            grouped("both", 1, nx, both, store_w, 0)
        with jax.named_scope("arrive_up"):
            arrive(w_tag, XU, YU)
        with jax.named_scope("late"):
            w_ref[1, pl.ds(PAD - 1, 1)] = yrecv[w_tag, 0, pl.ds(0, 1)]
            store_w(0, both(0, 0)[1])
            head = pl.ds(0, 1)
            owed_f = yrecv[8, 0] * yrecv[w_tag, 0]
            owed_d = yrecv[7, 0] * yrecv[w_tag, 0]
            owed = on_f * owed_f + on_d * owed_d
            for x in range(1, nx):
                if final:
                    out_w[x, head] += owed[x:x + 1]
                else:
                    fw[step][x, head] += owed_f[x:x + 1]
                    dw[step][x, head] += owed_d[x:x + 1]

        with jax.named_scope("allsums"):
            m0, m1, m2, m3 = read_sums(step)
        alpha = m0 / m1
        rr = alpha * alpha * m2 - m0
        ratio = rr / m0
        product = m1 - 2.0 * alpha * m2 + alpha * alpha * m3
        alpha_next = rr / (product - ratio * rr / alpha)
        on_r = alpha + alpha_next * (1.0 + ratio)
        on_w = -alpha_next * alpha
        weights.append((on_r, on_w))

        def following(x, low, rows, step=step, on_r=on_r, on_w=on_w, on_f=on_f, on_d=on_d):
            at, mid = pl.ds(PAD + low, rows), pl.ds(low, rows)
            r, w = fields[1 + step][x + 1, at], fields[4 + step][x + 1, at]
            advected = on_r * fr[step][x, mid] + on_w * fw[step][x, mid]
            diffused = (on_r / implicit_diagonal) * (r - w) + on_w * dw[step][x, mid]
            total = base[x, mid]
            total += on_f * advected + on_d * diffused
            return total, (advected, diffused)

    out_scale[...] = jnp.concatenate(weights[-1], axis=0)
    with jax.named_scope("sends"):
        for xu, yu in statics:
            pl.when(high_x)(xu.wait_send)
            pl.when(high_y)(yu.wait_send)
        for tag in range(7):
            sent(tag)
        for step in range(3):
            for copy, toward, _ in corners(step):
                pl.when(toward)(copy.wait_send)
            all_sums(step).wait_send()


def finish(base, on_r, on_w, scale, out_hbm, out, sem):
    nx = base.shape[0]
    chunks = CHUNKS if nx % CHUNKS == 0 else 1
    piece = nx // chunks
    copies = []
    for chunk in range(chunks):
        at = pl.ds(chunk * piece, piece)
        for x in range(chunk * piece, (chunk + 1) * piece):
            out[x] = base[x] + scale[:1] * on_r[x] + scale[1:] * on_w[x]
        copies.append(pltpu.make_async_copy(out.at[at], out_hbm.at[at], sem.at[chunk]))
        copies[-1].start()
    for copy in copies:
        copy.wait()


def local(gx, gy, cotangent, speed, coeff, dirs):
    nx, ny, nz = cotangent.shape
    f32 = jnp.float32
    rows = ny + 2 * PAD
    plain = pltpu.VMEM((nx, ny, nz), f32)
    dma = pltpu.SemaphoreType.DMA
    far = pl.BlockSpec(memory_space=pltpu.HBM)
    hbm = [pltpu.with_memory_space_constraint(v, pltpu.HBM) for v in (cotangent, speed, coeff, dirs)]
    whole = jax.ShapeDtypeStruct((nx, ny, nz), f32)
    total, on_r, on_w, scale = pl.pallas_call(
        functools.partial(kernel, gx, gy),
        out_shape=(whole, whole, whole, jax.ShapeDtypeStruct((2, nz), f32)),
        in_specs=[far] * 4,
        out_specs=(pl.BlockSpec(memory_space=pltpu.VMEM),) * 4,
        scratch_shapes=[
            *[pltpu.VMEM((nx + 2, rows, nz), f32)] * 7,
            *[plain] * 6,
            plain,
            pltpu.VMEM((nx + 1, ny, nz), f32),
            pltpu.VMEM((nx, rows, nz), f32),
            plain, plain,
            plain, plain, plain,
            pltpu.VMEM((nx + 1, ny, nz), f32),
            pltpu.VMEM((nx, rows, nz), f32),
            plain,
            plain, plain,
            pltpu.VMEM((9, 2, nx, nz), f32),
            pltpu.VMEM((9, 2, nx, nz), f32),
            pltpu.VMEM(dirs.shape, dirs.dtype),
            pltpu.VMEM((2, ny, nz), f32),
            pltpu.VMEM((ny, nz), f32),
            pltpu.VMEM((ny, nz), f32),
            pltpu.VMEM((nx, 8, nz), f32),
            pltpu.VMEM((nx, 8, nz), f32),
            pltpu.VMEM((2, ny, nz), f32),
            pltpu.VMEM((3, ny, nz), f32),
            pltpu.VMEM((3, nx, nz), f32),
            pltpu.VMEM((7, nx, nz), f32),
            pltpu.VMEM((3, 4, 1, nz), f32),
            pltpu.VMEM((3, 4, 1, nz), f32),
            pltpu.VMEM((3, gx * gy, 1, nz), f32),
            dma((8 + 6 * CHUNKS,)), dma((9, 4)), dma((9, 4)),
            dma((3, 3)), dma((3, 3)), dma((3,)), dma((3,)),
            pltpu.SemaphoreType.REGULAR((max(gx, gy).bit_length(),)),
        ],
        compiler_params=pltpu.CompilerParams(
            collective_id=0, has_side_effects=True, vmem_limit_bytes=46 * 1024 * 1024
        ),
    )(*hbm)
    return pl.pallas_call(
        finish,
        out_shape=whole,
        in_specs=[pl.BlockSpec(memory_space=pltpu.VMEM)] * 4,
        out_specs=pl.BlockSpec(memory_space=pltpu.HBM),
        scratch_shapes=[plain, dma((CHUNKS,))],
        compiler_params=pltpu.CompilerParams(vmem_limit_bytes=8 * 1024 * 1024),
    )(total, on_r, on_w, scale)


def solution(mesh):
    return jax.shard_map(
        functools.partial(local, mesh.shape["gx"], mesh.shape["gy"]),
        mesh=mesh,
        in_specs=(
            P("gx", "gy", None),
            P(None, "gx", "gy", None),
            P(None, "gx", "gy", None),
            P(None, "gx", "gy"),
        ),
        out_specs=P("gx", "gy", None),
        check_vma=False,
    )
```

```python
import functools

import jax
import jax.numpy as jnp
from jax import lax
from jax.experimental import pallas as pl
from jax.experimental.pallas import tpu as pltpu
from jax.sharding import PartitionSpec as P

explicit_table = (
    (0.0, 0.0, 0.0, 0.0),
    (0.5, 0.0, 0.0, 0.0),
    (0.25, 0.5, 0.0, 0.0),
    (0.2, 0.3, 0.5, 0.0),
)
implicit_table = (
    (0.0, 0.0, 0.0, 0.0),
    (0.25, 0.25, 0.0, 0.0),
    (0.25, 0.25, 0.25, 0.0),
    (0.15, 0.35, 0.25, 0.25),
)
section_weights = (0.15, 0.35, 0.25, 0.25)
implicit_diagonal = 0.25

MESH = pl.DeviceIdType.MESH
PAD = 8


GROUP = {"masks": 8, "diagonals": 8, "source": 16, "strip": 29, "next": 29, "image": 10, "energy": 14, "rim": 28, "carry": 16, "both": 8, "gather": 16, "last": 8}
CHUNKS = 4


def grouped(name, low, high, value, store, carry):
    size = GROUP[name]

    def group(planes, carry):
        found = []
        for x in planes:
            carry, kept = value(x, carry)
            found.append(kept)
        for x, kept in zip(planes, found):
            store(x, kept)
        return carry

    turns = (high - low) // size
    carry = lax.fori_loop(
        0, turns, lambda t, c: group([low + t * size + k for k in range(size)], c), carry)
    rest = list(range(low + turns * size, high))
    return group(rest, carry) if rest else carry


def kernel(
    gx, gy, cot_hbm, speed_hbm, coeff_hbm, dirs_hbm, out_base, out_r, out_w, out_scale,
    f0, f1, f2, f3, f4, f5, f6, fr0, fr1, fw0, fw1, dw0, dw1, base, cx, cy, cz, czm, px, py, pz, mx, my, mz, gdiag, fdiag,
    ysend, yrecv, dirs_ref, c_ends, cx_top, mx_top, cy_top, py_top, landed, wpart, ypart, yside, corner_out, corner_in, slots,
    load_sem, send_sem, recv_sem, corner_send, corner_recv, sum_send, sum_recv, known,
):
    nx, ny, nz = out_base.shape
    fields = (f0, f1, f2, f3, f4, f5, f6)
    fr, fw, dw = (fr0, fr1), (fw0, fw1), (dw0, dw1)
    me_x, me_y = lax.axis_index("gx"), lax.axis_index("gy")
    count = gx * gy
    me = me_x * gy + me_y
    own = pl.ds(PAD, ny)
    up = pl.ds(PAD + 1, ny)
    down = pl.ds(PAD - 1, ny)
    lane = lax.broadcasted_iota(jnp.int32, (ny, nz), 1)
    last_lane = lane == nz - 1
    low_x, low_y = me_x > 0, me_y > 0
    high_x, high_y = me_x < gx - 1, me_y < gy - 1

    def ahead_z(v):
        return pltpu.roll(v, nz - 1, 1)

    def behind_z(v):
        return pltpu.roll(v, 1, 1)

    chunks = CHUNKS if nx % CHUNKS == 0 else 1
    piece = nx // chunks

    def load(k, src, dst):
        copy = pltpu.make_async_copy(src, dst, load_sem.at[k])
        copy.start()
        return copy

    def greet(sem, d):
        for dx in (-d, 0, d):
            for dy in (-d, 0, d):
                if (dx, dy) == (0, 0) or abs(dx) >= gx or abs(dy) >= gy:
                    continue
                x, y = me_x + dx, me_y + dy
                there = jnp.logical_and(jnp.logical_and(x >= 0, x < gx), jnp.logical_and(y >= 0, y < gy))

                @pl.when(there)
                def _():
                    pl.semaphore_signal(sem, inc=1, device_id={"gx": x, "gy": y}, device_id_type=MESH)

    def greeted(sem, d):
        def near(at, size):
            return 1 + (at >= d).astype(jnp.int32) + (at + d < size).astype(jnp.int32)

        pl.semaphore_wait(sem, near(me_x, gx) * near(me_y, gy) - 1)

    reach = [1]
    while 2 * reach[-1] < max(gx, gy):
        reach.append(2 * reach[-1])

    def pass_on(k, last=False):
        while k < len(reach):
            greeted(known.at[k], reach[k])
            k += 1
            if k < len(reach):
                greet(known.at[k], reach[k])
            if not last:
                break

    with jax.named_scope("loads"):
        plane = jnp.zeros((ny, nz), jnp.float32)
        for k in range(7):
            fields[k][0, own] = plane
            fields[k][nx + 1, own] = plane
        landed[0] = plane
        landed[1] = plane
        yrecv[...] = jnp.zeros_like(yrecv)
        corner_in[...] = jnp.zeros_like(corner_in)

        barrier = pltpu.get_barrier_semaphore()
        greet(barrier, 1)

        first = 2 + 6 * chunks
        early = [
            load(first + 4, cot_hbm.at[0], c_ends.at[0]),
            load(first + 5, cot_hbm.at[nx - 1], c_ends.at[1]),
            load(1 + 6 * chunks, dirs_hbm, dirs_ref),
        ]
        tops = [
            load(first, coeff_hbm.at[0, nx - 1], cx_top),
            load(first + 1, speed_hbm.at[0, nx - 1], mx_top),
            load(first + 2, coeff_hbm.at[1, :, pl.ds(ny - 8, 8)], cy_top),
            load(first + 3, speed_hbm.at[1, :, pl.ds(ny - 8, 8)], py_top),
        ]
        cot_load = load(0, cot_hbm, fields[0].at[pl.ds(1, nx), own])
        loads = []
        for chunk in range(chunks):
            at = pl.ds(chunk * piece, piece)
            loads.append([
                load(1 + 6 * chunk + k, src, dst)
                for k, (src, dst) in enumerate((
                    (coeff_hbm.at[0, at], cx.at[pl.ds(1 + chunk * piece, piece)]),
                    (coeff_hbm.at[1, at], cy.at[at, own]),
                    (coeff_hbm.at[2, at], cz.at[at]),
                    (speed_hbm.at[0, at], px.at[at]),
                    (speed_hbm.at[1, at], py.at[at]),
                    (speed_hbm.at[2, at], pz.at[at]),
                ))
            ])

        cx[0] = plane
        mx[0] = plane

        def zero_rows(x, carry):
            cy[x, pl.ds(0, PAD)] = jnp.zeros((PAD, nz), jnp.float32)
            my[x, pl.ds(0, PAD)] = jnp.zeros((PAD, nz), jnp.float32)
            for k in range(7):
                fields[k][x + 1, pl.ds(0, PAD)] = jnp.zeros((PAD, nz), jnp.float32)
                fields[k][x + 1, pl.ds(PAD + ny, PAD)] = jnp.zeros((PAD, nz), jnp.float32)
            return carry

        lax.fori_loop(0, nx, zero_rows, 0)

    def channel(tag, k, src, dst, axis, move):
        size, at = (gx, me_x) if axis == "gx" else (gy, me_y)
        return pltpu.make_async_remote_copy(
            src, dst, send_sem.at[tag, k], recv_sem.at[tag, k],
            device_id={axis: lax.rem(at + size + move, size)}, device_id_type=MESH)

    def x_down(tag, src, dst):
        return channel(tag, 0, src, dst, "gx", -1)

    def x_up(tag, src, dst):
        return channel(tag, 1, src, dst, "gx", 1)

    def y_down(tag, src):
        return channel(tag, 2, src, yrecv.at[tag, 1], "gy", -1)

    def y_up(tag):
        return channel(tag, 3, ysend.at[tag, 1], yrecv.at[tag, 0], "gy", 1)

    def copies(tag):
        field = fields[tag]
        partial = tag > 3
        return (
            x_down(
                tag, wpart.at[tag - 4] if partial else field.at[1, own] if tag else c_ends.at[0], field.at[nx + 1, own]),
            x_up(tag, field.at[nx, own] if tag else c_ends.at[1], field.at[0, own]),
            y_down(tag, ypart.at[tag - 4] if partial else ysend.at[tag, 0]),
            y_up(tag),
        )

    starts = (low_x, high_x, low_y, high_y)
    ends = (high_x, low_x, high_y, low_y)

    def start(tag, *which):
        every = copies(tag)
        for k in which:
            pl.when(starts[k])(every[k].start)

    odd = lax.rem(me_x, 2) == 1

    def start_if(also, tag, k):
        pl.when(jnp.logical_and(also, starts[k]))(copies(tag)[k].start)

    def arrive(tag, *which):
        every = copies(tag)
        for k in which:
            pl.when(ends[k])(every[k].wait_recv)

    def sent(tag):
        for k, copy in enumerate(copies(tag)):
            pl.when(starts[k])(copy.wait_send)

    XD, XU, YD, YU = range(4)

    def corners(step):
        out = []
        for k, (rows, dx, dy) in enumerate(((pl.ds(0, 1), -1, 1), (pl.ds(1, 2), -1, -1), (pl.ds(3, 1), 1, -1))):
            to = {"gx": lax.rem(me_x + gx + dx, gx), "gy": lax.rem(me_y + gy + dy, gy)}
            copy = pltpu.make_async_remote_copy(
                corner_out.at[step, rows], corner_in.at[step, rows],
                corner_send.at[step, k], corner_recv.at[step, k], device_id=to, device_id_type=MESH)
            toward = [low_x if dx < 0 else high_x, low_y if dy < 0 else high_y]
            whence = [high_x if dx < 0 else low_x, high_y if dy < 0 else low_y]
            out.append((copy, jnp.logical_and(*toward), jnp.logical_and(*whence)))
        return out

    def unpack(tag):
        for x in range(nx):
            fields[tag][1 + x, pl.ds(PAD - 1, 1)] = yrecv[tag, 0, pl.ds(x, 1)]
            fields[tag][1 + x, pl.ds(PAD + ny, 1)] = yrecv[tag, 1, pl.ds(x, 1)]

    with jax.named_scope("barrier"):
        for copy in early + tops[:2]:
            copy.wait()
        dirs = [dirs_ref[d].astype(jnp.float32).T for d in range(3)]

        def upper(d, x):
            column = (lax.broadcasted_iota(jnp.int32, (nx, nz), 0) == x).astype(jnp.float32)
            return jnp.dot(dirs[d], column, preferred_element_type=jnp.float32) > 0.5

        mx_top[...] = jnp.where(upper(0, nx - 1), mx_top[...], 0.0)
        statics = (
            (x_up(7, cx_top, landed.at[0]), y_up(7)),
            (x_up(8, mx_top, landed.at[1]), y_up(8)),
        )
        greeted(barrier, 1)
        start(0, XD, XU)
        greet(known.at[0], reach[0])
        for xu, _ in statics:
            pl.when(high_x)(xu.start)
    with jax.named_scope("rows"):
        for copy in [cot_load] + tops[2:]:
            copy.wait()
        for x in range(nx):
            at = pl.ds(x, 1)
            ysend[0, 0, at] = fields[0][x + 1, pl.ds(PAD, 1)]
            ysend[0, 1, at] = fields[0][x + 1, pl.ds(PAD + ny - 1, 1)]
            ysend[7, 1, at] = cy_top[x, 7:]
            yside[6, at] = py_top[x, 7:]
        edge = jnp.broadcast_to(dirs_ref[1][:, ny - 1:], (nx, nz)) > 0
        ysend[8, 1] = jnp.where(edge, yside[6], 0.0)
        yside[6] = jnp.where(edge, 0.0, yside[6])
        start(0, YD, YU)
        for _, yu in statics:
            pl.when(high_y)(yu.start)

    def masks(x, carry):
        low = [jnp.where(upper(d, x), ref[x], 0.0) for d, ref in enumerate((px, py, pz))]
        return carry, (low, [ref[x] - m for m, ref in zip(low, (px, py, pz))], cz[x])

    def store_masks(x, kept):
        low, high, c = kept
        mx[x + 1] = low[0]
        my[x, own] = low[1]
        mz[x] = jnp.where(last_lane, 0.0, low[2])
        px[x], py[x] = high[0], high[1]
        pz[x] = high[2]
        czm[x] = jnp.where(last_lane, 0.0, c)

    def diagonals(x, carry):
        p = pz[x]
        f = px[x] + mx[x] + py[x] + my[x, down] + p + behind_z(mz[x])
        g = cx[x + 1] + cx[x] + cy[x, own] + cy[x, down] + cz[x] + behind_z(czm[x])
        return carry, (f, g, jnp.where(last_lane, 0.0, p))

    def store_diagonals(x, kept):
        fdiag[x], gdiag[x], pz[x] = kept

    for chunk in range(chunks):
        low, high = chunk * piece, (chunk + 1) * piece
        with jax.named_scope("loadwait"):
            for copy in loads[chunk]:
                copy.wait()
        with jax.named_scope("masks"):
            grouped("masks", low, high, masks, store_masks, 0)
        with jax.named_scope("diagonals"):
            grouped("diagonals", low, high, diagonals, store_diagonals, 0)

    pass_on(0)

    def spread(ref, x):
        v = ref[x + 1, own]
        total = cx[x + 1] * ref[x + 2, own] + cx[x] * ref[x, own]
        total += cy[x, own] * ref[x + 1, up] + cy[x, down] * ref[x + 1, down]
        c = czm[x]
        total += c * ahead_z(v) + behind_z(c * v)
        return v, total - gdiag[x] * v

    def inner(ref, x):
        v = ref[x + 1, own]
        total = cx[1] * ref[2, own] if x == 0 else cx[x] * ref[x, own]
        total += cy[x, own] * ref[x + 1, up] + cy[x, down] * ref[x + 1, down]
        c = czm[x]
        total += c * ahead_z(v) + behind_z(c * v)
        return v - implicit_diagonal * (total - gdiag[x] * v)

    def carried(ref, x):
        v = ref[x + 1, own]
        total = px[x] * ref[x + 2, own] + mx[x] * ref[x, own]
        total += py[x] * ref[x + 1, up] + my[x, down] * ref[x + 1, down]
        total += pz[x] * ahead_z(v) + behind_z(mz[x] * v)
        return total - fdiag[x] * v

    def fold(v):
        return jnp.sum(v.reshape(v.shape[0] // 8, 8, nz), axis=0)

    nothing = jnp.zeros((8, nz), jnp.float32)

    def keep(tag, x, v):
        fields[tag][x + 1, own] = v
        ysend[tag, 0, pl.ds(x, 1)] = v[:1]
        ysend[tag, 1, pl.ds(x, 1)] = v[ny - 1:]

    row_x = lax.broadcasted_iota(jnp.int32, (nx, nz), 0)
    between = jnp.logical_and(row_x > 0, row_x < nx - 1)
    across_x = jnp.where(high_x, implicit_diagonal, 0.0)
    across_y = jnp.where(high_y, implicit_diagonal, 0.0)

    square = (lax.broadcasted_iota(jnp.int32, (8, nz), 0) == lax.broadcasted_iota(jnp.int32, (8, nz), 1))

    def send_sums(step, sums):
        rows = [jnp.sum(m, axis=0, keepdims=True) for m in sums]
        rows = jnp.concatenate(rows + [jnp.zeros((8 - len(rows), nz), jnp.float32)], axis=0)
        totals = jnp.broadcast_to(jnp.sum(rows, axis=1, keepdims=True), (8, nz))
        slots[step, me] = jnp.sum(jnp.where(square, totals, 0.0), axis=0, keepdims=True)
        for off in range(1, count):
            to = {"gx": lax.rem(me_x + off // gy, gx), "gy": lax.rem(me_y + off % gy, gy)}
            pltpu.make_async_remote_copy(
                slots.at[step, me], slots.at[step, me], sum_send.at[step], sum_recv.at[step],
                device_id=to, device_id_type=MESH).start()

    def all_sums(step):
        some = slots.at[step, pl.ds(0, count - 1)]
        return pltpu.make_async_remote_copy(
            some, some, sum_send.at[step], sum_recv.at[step],
            device_id={"gx": lax.rem(me_x + 1, gx)}, device_id_type=MESH)

    def read_sums(step):
        all_sums(step).wait_recv()
        total = jnp.broadcast_to(jnp.sum(slots[step], axis=0), (8, nz))
        total = jnp.sum(jnp.where(square, total, 0.0), axis=1, keepdims=True)
        total = jnp.broadcast_to(total, (8, nz))
        return [total[k:k + 1] for k in range(4)]

    weights = []
    for step, section in enumerate((3, 2, 1)):
        r_tag, w_tag = 1 + step, 4 + step
        r_ref, w_ref = fields[r_tag], fields[w_tag]

        def first_pass(x, m0):
            if step == 0:
                c_ref = fields[0]
                r, more = section_weights[3] * (spread(c_ref, x)[1] + carried(c_ref, x)), None
            return m0 + fold(r * r), (r, more)

        def store_first(x, kept):
            r, more = kept
            keep(r_tag, x, r)
            yside[5, pl.ds(x, 1)] = r[1:2]

        def part(low, rows):
            at, mid = pl.ds(PAD + low, rows), pl.ds(low, rows)

            def value(x, m0):
                r, more = following(x, low, rows)
                return m0 + fold(r * r), (r, more)

            def store(x, kept):
                r, more = kept
                r_ref[x + 1, at] = r
                if low < 8:
                    ysend[r_tag, 0, pl.ds(x, 1)] = r[:1]
                    yside[5, pl.ds(x, 1)] = r[1:2]
                if low + rows == ny:
                    ysend[r_tag, 1, pl.ds(x, 1)] = r[rows - 1:]
                fr[step - 1][x, mid], dw[step - 1][x, mid] = more

            return value, store

        def send_x():
            corner = r_ref[1, pl.ds(PAD, 1)]
            corner_out[step, 0] = cy[0, pl.ds(PAD + ny - 1, 1)] * r_ref[1, pl.ds(PAD + ny - 1, 1)]
            corner_out[step, 1] = cy[0, pl.ds(PAD - 1, 1)] * corner
            corner_out[step, 2] = cx[0, pl.ds(0, 1)] * corner
            corner_out[step, 3] = cx[nx, pl.ds(0, 1)] * r_ref[nx, pl.ds(PAD, 1)]
            for copy, toward, _ in corners(step):
                pl.when(toward)(copy.start)
            start_if(True, r_tag, XD)
            start_if(odd, r_tag, XU)
            wpart[step] = inner(r_ref, 0)
            start_if(jnp.logical_not(odd), w_tag, XD)
            start_if(jnp.logical_not(odd), r_tag, XU)

        outer = (0, 1, nx - 1)
        m0 = nothing
        if step == 0:
            with jax.named_scope("first"):
                m0 = grouped("source", 1, nx - 1, first_pass, store_first, m0)
            with jax.named_scope("arrive0"):
                arrive(0, XD, XU, YD, YU)
                m0, kept = first_pass(nx - 1, m0)
                store_first(nx - 1, kept)
                fields[0][1, pl.ds(PAD - 1, 1)] = yrecv[0, 0, pl.ds(0, 1)]
                fields[0][1, pl.ds(PAD + ny, 1)] = yrecv[0, 1, pl.ds(0, 1)]
            with jax.named_scope("statics"):
                for xu, yu in statics:
                    pl.when(low_x)(xu.wait_recv)
                    pl.when(low_y)(yu.wait_recv)
            head = pl.ds(0, 1)
            with jax.named_scope("firstedge"):
                for side, change in (
                    (0, (yrecv[7, 0] + yrecv[8, 0]) * (yrecv[0, 0] - ysend[0, 0])),
                    (1, (ysend[7, 1] + yside[6]) * yrecv[0, 1]),
                ):
                    change = jnp.where(row_x > 0, section_weights[3] * change, 0.0)
                    r = jnp.where(row_x > 0, ysend[r_tag, side], 0.0)
                    m0 += fold((2.0 * r + change) * change)
                    ysend[r_tag, side] = r + change
                for x in range(1, nx):
                    r_ref[1 + x, pl.ds(PAD, 1)] = ysend[r_tag, 0, pl.ds(x, 1)]
                    r_ref[1 + x, pl.ds(PAD + ny - 1, 1)] = ysend[r_tag, 1, pl.ds(x, 1)]
                cx[0] = landed[0]
                mx[0] = landed[1]
                gdiag[0] += cx[0]
                fdiag[0] += mx[0]
                cy[0, pl.ds(PAD - 1, 1)] = yrecv[7, 0, head]
                my[0, pl.ds(PAD - 1, 1)] = yrecv[8, 0, head]
                gdiag[0, head] += yrecv[7, 0, head]
                fdiag[0, head] += yrecv[8, 0, head]
                m0, kept = first_pass(0, m0)
                store_first(0, kept)
                send_x()
                start(r_tag, YD, YU)
            with jax.named_scope("patch"):
                for x in range(nx):
                    at = pl.ds(x, 1)
                    if x:
                        row = yrecv[7, 0, at]
                        cy[x, pl.ds(PAD - 1, 1)] = row
                        gdiag[x, head] += row
                        row = yrecv[8, 0, at]
                        my[x, pl.ds(PAD - 1, 1)] = row
                        fdiag[x, head] += row
                    yside[3, at] = gdiag[x, head]
                    yside[0, at] = cx[x + 1, head] if x < nx - 1 else jnp.zeros((1, nz), jnp.float32)
                    yside[4, at] = cx[x, head] if x else jnp.zeros((1, nz), jnp.float32)
                    yside[1, at] = cy[x, pl.ds(PAD, 1)]
                    yside[2, at] = czm[x, head]
        else:
            with jax.named_scope("firstedge"):
                value, store = part(0, ny)
                for x in outer:
                    m0, kept = value(x, m0)
                    store(x, kept)
                send_x()
            with jax.named_scope("strips"):
                for low in (0, ny - 8):
                    value, store = part(low, 8)
                    m0 = grouped("strip", 2, nx - 1, value, store, m0)
                start(r_tag, YD, YU)
        with jax.named_scope("corners"):
            v = ysend[r_tag, 0]
            c = yside[2]
            total = yside[0] * pltpu.roll(v, nx - 1, 0) + yside[4] * pltpu.roll(v, 1, 0)
            total += yside[1] * yside[5] + c * ahead_z(v) + behind_z(c * v)
            ypart[step] = v - implicit_diagonal * (total - yside[3] * v)
            start(w_tag, YD)
            start_if(odd, w_tag, XD)
        if step:
            value, store = part(8, ny - 16)
            with jax.named_scope("first"):
                m0 = grouped("next", 2, nx - 1, value, store, m0)

        def second_pass(x, sums):
            m1, m2 = sums
            r, d = spread(r_ref, x)
            w = r - implicit_diagonal * d
            return (m1 + fold(r * w), m2 + fold(w * w)), w

        def store_second(x, w):
            keep(w_tag, x, w)

        if step == 0:
            pass_on(1)
        with jax.named_scope("image"):
            sums = grouped("image", 1, nx - 1, second_pass, store_second, (nothing, nothing))

        def energy(x, low, rows):
            at, above = pl.ds(PAD + low, rows), pl.ds(PAD + low + 1, rows)
            mid = pl.ds(low, rows)
            w = w_ref[x + 1, at]
            jump_x = w_ref[x + 2, at] - w
            jump_y = w_ref[x + 1, above] - w
            jump_z = jnp.where(last_lane[:rows], 0.0, ahead_z(w)) - w
            total = cx[x + 1, mid] * jump_x * jump_x + cy[x, at] * jump_y * jump_y
            return fold(total + cz[x, mid] * jump_z * jump_z)

        with jax.named_scope("energy"):
            m3 = grouped("energy", 1, nx - 2, lambda x, m: (m + energy(x, 8, ny - 16), None), lambda x, kept: None, nothing)

        with jax.named_scope("arrive_y"):
            arrive(r_tag, YD, YU)
        with jax.named_scope("yfix"):
            unpack(r_tag)
            m1, m2 = sums
            for side, face in ((0, yrecv[7, 0]), (1, ysend[7, 1])):
                change = jnp.where(between, -implicit_diagonal * face * yrecv[r_tag, side], 0.0)
                w = ysend[w_tag, side]
                ysend[w_tag, side] = w + change
                m1 += fold(ysend[r_tag, side] * change)
                m2 += fold((2.0 * w + change) * change)
            for x in range(1, nx - 1):
                w_ref[1 + x, pl.ds(PAD, 1)] = ysend[w_tag, 0, pl.ds(x, 1)]
                w_ref[1 + x, pl.ds(PAD + ny - 1, 1)] = ysend[w_tag, 1, pl.ds(x, 1)]
        with jax.named_scope("rim"):
            m3 = grouped(
                "rim", 1, nx - 2, lambda x, m: (m + energy(x, 0, 8) + energy(x, ny - 8, 8), None), lambda x, kept: None, m3)
        with jax.named_scope("arrive_x"):
            arrive(r_tag, XD, XU)
        with jax.named_scope("edges"):
            sums = (m1, m2)
            for x in (0, nx - 1):
                sums, w = second_pass(x, sums)
                store_second(x, w)
            m1, m2 = sums
        with jax.named_scope("arrive_w"):
            arrive(w_tag, XD, YD)
            for copy, _, whence in corners(step):
                pl.when(whence)(copy.wait_recv)
        with jax.named_scope("close"):
            w_ref[nx + 1, own] = w_ref[nx + 1, own] - across_x * (cx[nx] * r_ref[nx, own])
            for k, y in ((0, 0), (1, ny - 1)):
                w_ref[nx + 1, pl.ds(PAD + y, 1)] -= implicit_diagonal * corner_in[step, k]
            above = yrecv[w_tag, 1] - across_y * (ysend[7, 1] * ysend[r_tag, 1])
            above -= jnp.where(row_x == 0, implicit_diagonal * corner_in[step, 3], 0.0)
            above -= jnp.where(row_x == nx - 1, implicit_diagonal * corner_in[step, 2], 0.0)
            for x in (0, nx - 2, nx - 1):
                m3 += energy(x, 0, ny)
            m3 += fold(ysend[7, 1] * above * (above - 2.0 * ysend[w_tag, 1]))
            m3 = m2 + implicit_diagonal * m3
        with jax.named_scope("sendsums"):
            if step == 0:
                pass_on(2, last=True)
            send_sums(step, (m0, m1, m2, m3))
            start(w_tag, YU, XU)
            for x in range(nx):
                w_ref[1 + x, pl.ds(PAD + ny, 1)] = above[x:x + 1]

        target = section - 1
        final = target == 0
        on_f, on_d = explicit_table[section][target], implicit_table[section][target]

        def carry(x, c):
            f = carried(r_ref, x)
            if final:
                r = r_ref[x + 1, own]
                f = on_f * f + ((on_d / implicit_diagonal) * (r - w_ref[x + 1, own]) + r)
            return c, f

        def store_r(x, kept):
            (out_r if final else fr[step])[x] = kept

        with jax.named_scope("carry"):
            grouped("carry", 0, nx, carry, store_r, 0)

        share = section_weights[target] / section_weights[3]

        def gather(x, c):
            total = share * fields[1][x + 1, own]
            for k in range(step):
                total += explicit_table[3 - k][target] * fr[k][x] + implicit_table[3 - k][target] * dw[k][x]
            if target == 0:
                total += fields[0][x + 1, own]
                for k in range(step):
                    on_r, on_w = weights[k]
                    total += on_r * fields[1 + k][x + 1, own] + on_w * fields[4 + k][x + 1, own]
            return c, total

        def store_base(x, kept):
            (out_base if final else base)[x] = kept

        with jax.named_scope("gather"):
            grouped("gather", 0, nx, gather, store_base, 0)

        def store_w(x, kept):
            if final:
                out_w[x] = kept
            else:
                fw[step][x], dw[step][x] = kept

        def both(x, c):
            f, (w, d) = carried(w_ref, x), spread(w_ref, x)
            return c, on_f * f + on_d * d + w if final else (f, d)

        with jax.named_scope("both"):
            grouped("both", 1, nx, both, store_w, 0)
        with jax.named_scope("arrive_up"):
            arrive(w_tag, XU, YU)
        with jax.named_scope("late"):
            w_ref[1, pl.ds(PAD - 1, 1)] = yrecv[w_tag, 0, pl.ds(0, 1)]
            store_w(0, both(0, 0)[1])
            head = pl.ds(0, 1)
            owed_f = yrecv[8, 0] * yrecv[w_tag, 0]
            owed_d = yrecv[7, 0] * yrecv[w_tag, 0]
            owed = on_f * owed_f + on_d * owed_d
            for x in range(1, nx):
                if final:
                    out_w[x, head] += owed[x:x + 1]
                else:
                    fw[step][x, head] += owed_f[x:x + 1]
                    dw[step][x, head] += owed_d[x:x + 1]

        with jax.named_scope("allsums"):
            m0, m1, m2, m3 = read_sums(step)
        alpha = m0 / m1
        beyond = m1 / m0
        rr = alpha * alpha * m2 - m0
        ratio = rr * (1.0 / m0)
        product = m1 - 2.0 * alpha * m2 + alpha * alpha * m3
        alpha_next = rr / (product - ratio * rr * beyond)
        on_r = alpha + alpha_next * (1.0 + ratio)
        on_w = -alpha_next * alpha
        weights.append((on_r, on_w))

        def following(x, low, rows, step=step, on_r=on_r, on_w=on_w, on_f=on_f, on_d=on_d):
            at, mid = pl.ds(PAD + low, rows), pl.ds(low, rows)
            r, w = fields[1 + step][x + 1, at], fields[4 + step][x + 1, at]
            advected = on_r * fr[step][x, mid] + on_w * fw[step][x, mid]
            diffused = (on_r / implicit_diagonal) * (r - w) + on_w * dw[step][x, mid]
            total = base[x, mid]
            total += on_f * advected + on_d * diffused
            return total, (advected, diffused)

    out_scale[...] = jnp.concatenate(weights[-1], axis=0)
    with jax.named_scope("sends"):
        for xu, yu in statics:
            pl.when(high_x)(xu.wait_send)
            pl.when(high_y)(yu.wait_send)
        for tag in range(7):
            sent(tag)
        for step in range(3):
            for copy, toward, _ in corners(step):
                pl.when(toward)(copy.wait_send)
            all_sums(step).wait_send()


def finish(base, on_r, on_w, scale, out_hbm, out, sem):
    nx = base.shape[0]
    chunks = CHUNKS if nx % CHUNKS == 0 else 1
    piece = nx // chunks
    copies = []
    for chunk in range(chunks):
        at = pl.ds(chunk * piece, piece)
        for x in range(chunk * piece, (chunk + 1) * piece):
            out[x] = base[x] + scale[:1] * on_r[x] + scale[1:] * on_w[x]
        copies.append(pltpu.make_async_copy(out.at[at], out_hbm.at[at], sem.at[chunk]))
        copies[-1].start()
    for copy in copies:
        copy.wait()


def local(gx, gy, cotangent, speed, coeff, dirs):
    nx, ny, nz = cotangent.shape
    f32 = jnp.float32
    rows = ny + 2 * PAD
    plain = pltpu.VMEM((nx, ny, nz), f32)
    dma = pltpu.SemaphoreType.DMA
    far = pl.BlockSpec(memory_space=pltpu.HBM)
    hbm = [pltpu.with_memory_space_constraint(v, pltpu.HBM) for v in (cotangent, speed, coeff, dirs)]
    whole = jax.ShapeDtypeStruct((nx, ny, nz), f32)
    total, on_r, on_w, scale = pl.pallas_call(
        functools.partial(kernel, gx, gy),
        out_shape=(whole, whole, whole, jax.ShapeDtypeStruct((2, nz), f32)),
        in_specs=[far] * 4,
        out_specs=(pl.BlockSpec(memory_space=pltpu.VMEM),) * 4,
        scratch_shapes=[
            *[pltpu.VMEM((nx + 2, rows, nz), f32)] * 7,
            *[plain] * 6,
            plain,
            pltpu.VMEM((nx + 1, ny, nz), f32),
            pltpu.VMEM((nx, rows, nz), f32),
            plain, plain,
            plain, plain, plain,
            pltpu.VMEM((nx + 1, ny, nz), f32),
            pltpu.VMEM((nx, rows, nz), f32),
            plain,
            plain, plain,
            pltpu.VMEM((9, 2, nx, nz), f32),
            pltpu.VMEM((9, 2, nx, nz), f32),
            pltpu.VMEM(dirs.shape, dirs.dtype),
            pltpu.VMEM((2, ny, nz), f32),
            pltpu.VMEM((ny, nz), f32),
            pltpu.VMEM((ny, nz), f32),
            pltpu.VMEM((nx, 8, nz), f32),
            pltpu.VMEM((nx, 8, nz), f32),
            pltpu.VMEM((2, ny, nz), f32),
            pltpu.VMEM((3, ny, nz), f32),
            pltpu.VMEM((3, nx, nz), f32),
            pltpu.VMEM((7, nx, nz), f32),
            pltpu.VMEM((3, 4, 1, nz), f32),
            pltpu.VMEM((3, 4, 1, nz), f32),
            pltpu.VMEM((3, gx * gy, 1, nz), f32),
            dma((8 + 6 * CHUNKS,)), dma((9, 4)), dma((9, 4)),
            dma((3, 3)), dma((3, 3)), dma((3,)), dma((3,)),
            pltpu.SemaphoreType.REGULAR((max(gx, gy).bit_length(),)),
        ],
        compiler_params=pltpu.CompilerParams(
            collective_id=0, has_side_effects=True, vmem_limit_bytes=46 * 1024 * 1024
        ),
    )(*hbm)
    return pl.pallas_call(
        finish,
        out_shape=whole,
        in_specs=[pl.BlockSpec(memory_space=pltpu.VMEM)] * 4,
        out_specs=pl.BlockSpec(memory_space=pltpu.HBM),
        scratch_shapes=[plain, dma((CHUNKS,))],
        compiler_params=pltpu.CompilerParams(vmem_limit_bytes=8 * 1024 * 1024),
    )(total, on_r, on_w, scale)


def solution(mesh):
    return jax.shard_map(
        functools.partial(local, mesh.shape["gx"], mesh.shape["gy"]),
        mesh=mesh,
        in_specs=(
            P("gx", "gy", None),
            P(None, "gx", "gy", None),
            P(None, "gx", "gy", None),
            P(None, "gx", "gy"),
        ),
        out_specs=P("gx", "gy", None),
        check_vma=False,
    )
```

```python
import functools

import jax
import jax.numpy as jnp
from jax import lax
from jax.experimental import pallas as pl
from jax.experimental.pallas import tpu as pltpu
from jax.sharding import PartitionSpec as P

explicit_table = (
    (0.0, 0.0, 0.0, 0.0),
    (0.5, 0.0, 0.0, 0.0),
    (0.25, 0.5, 0.0, 0.0),
    (0.2, 0.3, 0.5, 0.0),
)
implicit_table = (
    (0.0, 0.0, 0.0, 0.0),
    (0.25, 0.25, 0.0, 0.0),
    (0.25, 0.25, 0.25, 0.0),
    (0.15, 0.35, 0.25, 0.25),
)
section_weights = (0.15, 0.35, 0.25, 0.25)
implicit_diagonal = 0.25

MESH = pl.DeviceIdType.MESH
PAD = 8


GROUP = {"masks": 8, "diagonals": 8, "source": 10, "strip": 29, "next": 29, "image": 10, "energy": 14, "rim": 28, "carry": 16, "both": 8, "gather": 16, "last": 8}
CHUNKS = 4


def grouped(name, low, high, value, store, carry):
    size = GROUP[name]

    def group(planes, carry):
        found = []
        for x in planes:
            carry, kept = value(x, carry)
            found.append(kept)
        for x, kept in zip(planes, found):
            store(x, kept)
        return carry

    turns = (high - low) // size
    carry = lax.fori_loop(
        0, turns, lambda t, c: group([low + t * size + k for k in range(size)], c), carry)
    rest = list(range(low + turns * size, high))
    return group(rest, carry) if rest else carry


def kernel(
    gx, gy, cot_hbm, speed_hbm, coeff_hbm, dirs_hbm, out_base, out_r, out_w, out_scale,
    f0, f1, f2, f3, f4, f5, f6, fr0, fr1, fw0, fw1, dw0, dw1, base, cx, cy, cz, czm, px, py, pz, mx, my, mz, gdiag, fdiag,
    ysend, yrecv, dirs_ref, c_ends, cx_top, mx_top, cy_top, py_top, landed, wpart, ypart, yside, corner_out, corner_in, slots,
    load_sem, send_sem, recv_sem, corner_send, corner_recv, sum_send, sum_recv, known,
):
    nx, ny, nz = out_base.shape
    fields = (f0, f1, f2, f3, f4, f5, f6)
    fr, fw, dw = (fr0, fr1), (fw0, fw1), (dw0, dw1)
    me_x, me_y = lax.axis_index("gx"), lax.axis_index("gy")
    count = gx * gy
    me = me_x * gy + me_y
    own = pl.ds(PAD, ny)
    up = pl.ds(PAD + 1, ny)
    down = pl.ds(PAD - 1, ny)
    lane = lax.broadcasted_iota(jnp.int32, (ny, nz), 1)
    last_lane = lane == nz - 1
    low_x, low_y = me_x > 0, me_y > 0
    high_x, high_y = me_x < gx - 1, me_y < gy - 1

    def ahead_z(v):
        return pltpu.roll(v, nz - 1, 1)

    def behind_z(v):
        return pltpu.roll(v, 1, 1)

    chunks = CHUNKS if nx % CHUNKS == 0 else 1
    piece = nx // chunks

    def load(k, src, dst):
        copy = pltpu.make_async_copy(src, dst, load_sem.at[k])
        copy.start()
        return copy

    def greet(sem, d):
        for dx in (-d, 0, d):
            for dy in (-d, 0, d):
                if (dx, dy) == (0, 0) or abs(dx) >= gx or abs(dy) >= gy:
                    continue
                x, y = me_x + dx, me_y + dy
                there = jnp.logical_and(jnp.logical_and(x >= 0, x < gx), jnp.logical_and(y >= 0, y < gy))

                @pl.when(there)
                def _():
                    pl.semaphore_signal(sem, inc=1, device_id={"gx": x, "gy": y}, device_id_type=MESH)

    def greeted(sem, d):
        def near(at, size):
            return 1 + (at >= d).astype(jnp.int32) + (at + d < size).astype(jnp.int32)

        pl.semaphore_wait(sem, near(me_x, gx) * near(me_y, gy) - 1)

    reach = [1]
    while 2 * reach[-1] < max(gx, gy):
        reach.append(2 * reach[-1])

    def pass_on(k, last=False):
        while k < len(reach):
            greeted(known.at[k], reach[k])
            k += 1
            if k < len(reach):
                greet(known.at[k], reach[k])
            if not last:
                break

    with jax.named_scope("loads"):
        plane = jnp.zeros((ny, nz), jnp.float32)
        for k in range(7):
            fields[k][0, own] = plane
            fields[k][nx + 1, own] = plane
        landed[0] = plane
        landed[1] = plane
        yrecv[...] = jnp.zeros_like(yrecv)
        corner_in[...] = jnp.zeros_like(corner_in)

        barrier = pltpu.get_barrier_semaphore()
        greet(barrier, 1)

        first = 2 + 6 * chunks
        early = [
            load(first + 4, cot_hbm.at[0], c_ends.at[0]),
            load(first + 5, cot_hbm.at[nx - 1], c_ends.at[1]),
            load(1 + 6 * chunks, dirs_hbm, dirs_ref),
        ]
        tops = [
            load(first, coeff_hbm.at[0, nx - 1], cx_top),
            load(first + 1, speed_hbm.at[0, nx - 1], mx_top),
            load(first + 2, coeff_hbm.at[1, :, pl.ds(ny - 8, 8)], cy_top),
            load(first + 3, speed_hbm.at[1, :, pl.ds(ny - 8, 8)], py_top),
        ]
        cot_load = load(0, cot_hbm, fields[0].at[pl.ds(1, nx), own])
        loads = []
        for chunk in range(chunks):
            at = pl.ds(chunk * piece, piece)
            loads.append([
                load(1 + 6 * chunk + k, src, dst)
                for k, (src, dst) in enumerate((
                    (coeff_hbm.at[0, at], cx.at[pl.ds(1 + chunk * piece, piece)]),
                    (coeff_hbm.at[1, at], cy.at[at, own]),
                    (coeff_hbm.at[2, at], cz.at[at]),
                    (speed_hbm.at[0, at], px.at[at]),
                    (speed_hbm.at[1, at], py.at[at]),
                    (speed_hbm.at[2, at], pz.at[at]),
                ))
            ])

        cx[0] = plane
        mx[0] = plane

        def zero_rows(x, carry):
            cy[x, pl.ds(0, PAD)] = jnp.zeros((PAD, nz), jnp.float32)
            my[x, pl.ds(0, PAD)] = jnp.zeros((PAD, nz), jnp.float32)
            for k in range(7):
                fields[k][x + 1, pl.ds(0, PAD)] = jnp.zeros((PAD, nz), jnp.float32)
                fields[k][x + 1, pl.ds(PAD + ny, PAD)] = jnp.zeros((PAD, nz), jnp.float32)
            return carry

        lax.fori_loop(0, nx, zero_rows, 0)

    def channel(tag, k, src, dst, axis, move):
        size, at = (gx, me_x) if axis == "gx" else (gy, me_y)
        return pltpu.make_async_remote_copy(
            src, dst, send_sem.at[tag, k], recv_sem.at[tag, k],
            device_id={axis: lax.rem(at + size + move, size)}, device_id_type=MESH)

    def x_down(tag, src, dst):
        return channel(tag, 0, src, dst, "gx", -1)

    def x_up(tag, src, dst):
        return channel(tag, 1, src, dst, "gx", 1)

    def y_down(tag, src):
        return channel(tag, 2, src, yrecv.at[tag, 1], "gy", -1)

    def y_up(tag):
        return channel(tag, 3, ysend.at[tag, 1], yrecv.at[tag, 0], "gy", 1)

    def copies(tag):
        field = fields[tag]
        partial = tag > 3
        return (
            x_down(
                tag, wpart.at[tag - 4] if partial else field.at[1, own] if tag else c_ends.at[0], field.at[nx + 1, own]),
            x_up(tag, field.at[nx, own] if tag else c_ends.at[1], field.at[0, own]),
            y_down(tag, ypart.at[tag - 4] if partial else ysend.at[tag, 0]),
            y_up(tag),
        )

    starts = (low_x, high_x, low_y, high_y)
    ends = (high_x, low_x, high_y, low_y)

    def start(tag, *which):
        every = copies(tag)
        for k in which:
            pl.when(starts[k])(every[k].start)

    odd = lax.rem(me_x, 2) == 1

    def start_if(also, tag, k):
        pl.when(jnp.logical_and(also, starts[k]))(copies(tag)[k].start)

    def arrive(tag, *which):
        every = copies(tag)
        for k in which:
            pl.when(ends[k])(every[k].wait_recv)

    def sent(tag):
        for k, copy in enumerate(copies(tag)):
            pl.when(starts[k])(copy.wait_send)

    XD, XU, YD, YU = range(4)

    def corners(step):
        out = []
        for k, (rows, dx, dy) in enumerate(((pl.ds(0, 1), -1, 1), (pl.ds(1, 2), -1, -1), (pl.ds(3, 1), 1, -1))):
            to = {"gx": lax.rem(me_x + gx + dx, gx), "gy": lax.rem(me_y + gy + dy, gy)}
            copy = pltpu.make_async_remote_copy(
                corner_out.at[step, rows], corner_in.at[step, rows],
                corner_send.at[step, k], corner_recv.at[step, k], device_id=to, device_id_type=MESH)
            toward = [low_x if dx < 0 else high_x, low_y if dy < 0 else high_y]
            whence = [high_x if dx < 0 else low_x, high_y if dy < 0 else low_y]
            out.append((copy, jnp.logical_and(*toward), jnp.logical_and(*whence)))
        return out

    def unpack(tag):
        for x in range(nx):
            fields[tag][1 + x, pl.ds(PAD - 1, 1)] = yrecv[tag, 0, pl.ds(x, 1)]
            fields[tag][1 + x, pl.ds(PAD + ny, 1)] = yrecv[tag, 1, pl.ds(x, 1)]

    with jax.named_scope("barrier"):
        for copy in early + tops[:2]:
            copy.wait()
        dirs = [dirs_ref[d].astype(jnp.float32).T for d in range(3)]

        def upper(d, x):
            column = (lax.broadcasted_iota(jnp.int32, (nx, nz), 0) == x).astype(jnp.float32)
            return jnp.dot(dirs[d], column, preferred_element_type=jnp.float32) > 0.5

        mx_top[...] = jnp.where(upper(0, nx - 1), mx_top[...], 0.0)
        statics = (
            (x_up(7, cx_top, landed.at[0]), y_up(7)),
            (x_up(8, mx_top, landed.at[1]), y_up(8)),
        )
        greeted(barrier, 1)
        start(0, XD, XU)
        greet(known.at[0], reach[0])
        for xu, _ in statics:
            pl.when(high_x)(xu.start)
    with jax.named_scope("rows"):
        for copy in [cot_load] + tops[2:]:
            copy.wait()
        for x in range(nx):
            at = pl.ds(x, 1)
            ysend[0, 0, at] = fields[0][x + 1, pl.ds(PAD, 1)]
            ysend[0, 1, at] = fields[0][x + 1, pl.ds(PAD + ny - 1, 1)]
            ysend[7, 1, at] = cy_top[x, 7:]
            yside[6, at] = py_top[x, 7:]
        edge = jnp.broadcast_to(dirs_ref[1][:, ny - 1:], (nx, nz)) > 0
        ysend[8, 1] = jnp.where(edge, yside[6], 0.0)
        yside[6] = jnp.where(edge, 0.0, yside[6])
        start(0, YD, YU)
        for _, yu in statics:
            pl.when(high_y)(yu.start)

    def masks(x, carry):
        low = [jnp.where(upper(d, x), ref[x], 0.0) for d, ref in enumerate((px, py, pz))]
        return carry, (low, [ref[x] - m for m, ref in zip(low, (px, py, pz))], cz[x])

    def store_masks(x, kept):
        low, high, c = kept
        mx[x + 1] = low[0]
        my[x, own] = low[1]
        mz[x] = jnp.where(last_lane, 0.0, low[2])
        px[x], py[x] = high[0], high[1]
        pz[x] = high[2]
        czm[x] = jnp.where(last_lane, 0.0, c)

    def diagonals(x, carry):
        p = pz[x]
        f = px[x] + mx[x] + py[x] + my[x, down] + p + behind_z(mz[x])
        g = cx[x + 1] + cx[x] + cy[x, own] + cy[x, down] + cz[x] + behind_z(czm[x])
        return carry, (f, g, jnp.where(last_lane, 0.0, p))

    def store_diagonals(x, kept):
        fdiag[x], gdiag[x], pz[x] = kept

    for chunk in range(chunks):
        low, high = chunk * piece, (chunk + 1) * piece
        with jax.named_scope("loadwait"):
            for copy in loads[chunk]:
                copy.wait()
        with jax.named_scope("masks"):
            grouped("masks", low, high, masks, store_masks, 0)
        with jax.named_scope("diagonals"):
            grouped("diagonals", low, high, diagonals, store_diagonals, 0)

    pass_on(0)

    def spread(ref, x):
        v = ref[x + 1, own]
        total = cx[x + 1] * ref[x + 2, own] + cx[x] * ref[x, own]
        total += cy[x, own] * ref[x + 1, up] + cy[x, down] * ref[x + 1, down]
        c = czm[x]
        total += c * ahead_z(v) + behind_z(c * v)
        return v, total - gdiag[x] * v

    def inner(ref, x):
        v = ref[x + 1, own]
        total = cx[1] * ref[2, own] if x == 0 else cx[x] * ref[x, own]
        total += cy[x, own] * ref[x + 1, up] + cy[x, down] * ref[x + 1, down]
        c = czm[x]
        total += c * ahead_z(v) + behind_z(c * v)
        return v - implicit_diagonal * (total - gdiag[x] * v)

    def carried(ref, x):
        v = ref[x + 1, own]
        total = px[x] * ref[x + 2, own] + mx[x] * ref[x, own]
        total += py[x] * ref[x + 1, up] + my[x, down] * ref[x + 1, down]
        total += pz[x] * ahead_z(v) + behind_z(mz[x] * v)
        return total - fdiag[x] * v

    def fold(v):
        return jnp.sum(v.reshape(v.shape[0] // 8, 8, nz), axis=0)

    nothing = jnp.zeros((8, nz), jnp.float32)

    def keep(tag, x, v):
        fields[tag][x + 1, own] = v
        ysend[tag, 0, pl.ds(x, 1)] = v[:1]
        ysend[tag, 1, pl.ds(x, 1)] = v[ny - 1:]

    row_x = lax.broadcasted_iota(jnp.int32, (nx, nz), 0)
    between = jnp.logical_and(row_x > 0, row_x < nx - 1)
    across_x = jnp.where(high_x, implicit_diagonal, 0.0)
    across_y = jnp.where(high_y, implicit_diagonal, 0.0)

    square = (lax.broadcasted_iota(jnp.int32, (8, nz), 0) == lax.broadcasted_iota(jnp.int32, (8, nz), 1))

    def send_sums(step, sums):
        rows = [jnp.sum(m, axis=0, keepdims=True) for m in sums]
        rows = jnp.concatenate(rows + [jnp.zeros((8 - len(rows), nz), jnp.float32)], axis=0)
        totals = jnp.broadcast_to(jnp.sum(rows, axis=1, keepdims=True), (8, nz))
        slots[step, me] = jnp.sum(jnp.where(square, totals, 0.0), axis=0, keepdims=True)
        for off in range(1, count):
            to = {"gx": lax.rem(me_x + off // gy, gx), "gy": lax.rem(me_y + off % gy, gy)}
            pltpu.make_async_remote_copy(
                slots.at[step, me], slots.at[step, me], sum_send.at[step], sum_recv.at[step],
                device_id=to, device_id_type=MESH).start()

    def all_sums(step):
        some = slots.at[step, pl.ds(0, count - 1)]
        return pltpu.make_async_remote_copy(
            some, some, sum_send.at[step], sum_recv.at[step],
            device_id={"gx": lax.rem(me_x + 1, gx)}, device_id_type=MESH)

    def read_sums(step):
        all_sums(step).wait_recv()
        total = jnp.broadcast_to(jnp.sum(slots[step], axis=0), (8, nz))
        total = jnp.sum(jnp.where(square, total, 0.0), axis=1, keepdims=True)
        total = jnp.broadcast_to(total, (8, nz))
        return [total[k:k + 1] for k in range(4)]

    weights = []
    for step, section in enumerate((3, 2, 1)):
        r_tag, w_tag = 1 + step, 4 + step
        r_ref, w_ref = fields[r_tag], fields[w_tag]

        def first_pass(x, m0):
            if step == 0:
                c_ref = fields[0]
                r, more = section_weights[3] * (spread(c_ref, x)[1] + carried(c_ref, x)), None
            return m0 + fold(r * r), (r, more)

        def store_first(x, kept):
            r, more = kept
            keep(r_tag, x, r)
            yside[5, pl.ds(x, 1)] = r[1:2]

        def part(low, rows):
            at, mid = pl.ds(PAD + low, rows), pl.ds(low, rows)

            def value(x, m0):
                r, more = following(x, low, rows)
                return m0 + fold(r * r), (r, more)

            def store(x, kept):
                r, more = kept
                r_ref[x + 1, at] = r
                if low < 8:
                    ysend[r_tag, 0, pl.ds(x, 1)] = r[:1]
                    yside[5, pl.ds(x, 1)] = r[1:2]
                if low + rows == ny:
                    ysend[r_tag, 1, pl.ds(x, 1)] = r[rows - 1:]
                fr[step - 1][x, mid], dw[step - 1][x, mid] = more

            return value, store

        def send_x():
            corner = r_ref[1, pl.ds(PAD, 1)]
            corner_out[step, 0] = cy[0, pl.ds(PAD + ny - 1, 1)] * r_ref[1, pl.ds(PAD + ny - 1, 1)]
            corner_out[step, 1] = cy[0, pl.ds(PAD - 1, 1)] * corner
            corner_out[step, 2] = cx[0, pl.ds(0, 1)] * corner
            corner_out[step, 3] = cx[nx, pl.ds(0, 1)] * r_ref[nx, pl.ds(PAD, 1)]
            for copy, toward, _ in corners(step):
                pl.when(toward)(copy.start)
            start_if(True, r_tag, XD)
            start_if(odd, r_tag, XU)
            wpart[step] = inner(r_ref, 0)
            start_if(jnp.logical_not(odd), w_tag, XD)
            start_if(jnp.logical_not(odd), r_tag, XU)

        outer = (0, 1, nx - 1)
        m0 = nothing
        if step == 0:
            with jax.named_scope("first"):
                m0 = grouped("source", 1, nx - 1, first_pass, store_first, m0)
            with jax.named_scope("arrive0"):
                arrive(0, XD, XU, YD, YU)
                m0, kept = first_pass(nx - 1, m0)
                store_first(nx - 1, kept)
                fields[0][1, pl.ds(PAD - 1, 1)] = yrecv[0, 0, pl.ds(0, 1)]
                fields[0][1, pl.ds(PAD + ny, 1)] = yrecv[0, 1, pl.ds(0, 1)]
            with jax.named_scope("statics"):
                for xu, yu in statics:
                    pl.when(low_x)(xu.wait_recv)
                    pl.when(low_y)(yu.wait_recv)
            head = pl.ds(0, 1)
            with jax.named_scope("firstedge"):
                for side, change in (
                    (0, (yrecv[7, 0] + yrecv[8, 0]) * (yrecv[0, 0] - ysend[0, 0])),
                    (1, (ysend[7, 1] + yside[6]) * yrecv[0, 1]),
                ):
                    change = jnp.where(row_x > 0, section_weights[3] * change, 0.0)
                    r = jnp.where(row_x > 0, ysend[r_tag, side], 0.0)
                    m0 += fold((2.0 * r + change) * change)
                    ysend[r_tag, side] = r + change
                for x in range(1, nx):
                    r_ref[1 + x, pl.ds(PAD, 1)] = ysend[r_tag, 0, pl.ds(x, 1)]
                    r_ref[1 + x, pl.ds(PAD + ny - 1, 1)] = ysend[r_tag, 1, pl.ds(x, 1)]
                cx[0] = landed[0]
                mx[0] = landed[1]
                gdiag[0] += cx[0]
                fdiag[0] += mx[0]
                cy[0, pl.ds(PAD - 1, 1)] = yrecv[7, 0, head]
                my[0, pl.ds(PAD - 1, 1)] = yrecv[8, 0, head]
                gdiag[0, head] += yrecv[7, 0, head]
                fdiag[0, head] += yrecv[8, 0, head]
                m0, kept = first_pass(0, m0)
                store_first(0, kept)
                send_x()
                start(r_tag, YD, YU)
            with jax.named_scope("patch"):
                for x in range(nx):
                    at = pl.ds(x, 1)
                    if x:
                        row = yrecv[7, 0, at]
                        cy[x, pl.ds(PAD - 1, 1)] = row
                        gdiag[x, head] += row
                        row = yrecv[8, 0, at]
                        my[x, pl.ds(PAD - 1, 1)] = row
                        fdiag[x, head] += row
                    yside[3, at] = gdiag[x, head]
                    yside[0, at] = cx[x + 1, head] if x < nx - 1 else jnp.zeros((1, nz), jnp.float32)
                    yside[4, at] = cx[x, head] if x else jnp.zeros((1, nz), jnp.float32)
                    yside[1, at] = cy[x, pl.ds(PAD, 1)]
                    yside[2, at] = czm[x, head]
        else:
            with jax.named_scope("firstedge"):
                value, store = part(0, ny)
                for x in outer:
                    m0, kept = value(x, m0)
                    store(x, kept)
                send_x()
            with jax.named_scope("strips"):
                for low in (0, ny - 8):
                    value, store = part(low, 8)
                    m0 = grouped("strip", 2, nx - 1, value, store, m0)
                start(r_tag, YD, YU)
        with jax.named_scope("corners"):
            v = ysend[r_tag, 0]
            c = yside[2]
            total = yside[0] * pltpu.roll(v, nx - 1, 0) + yside[4] * pltpu.roll(v, 1, 0)
            total += yside[1] * yside[5] + c * ahead_z(v) + behind_z(c * v)
            ypart[step] = v - implicit_diagonal * (total - yside[3] * v)
            start(w_tag, YD)
            start_if(odd, w_tag, XD)
        if step:
            value, store = part(8, ny - 16)
            with jax.named_scope("first"):
                m0 = grouped("next", 2, nx - 1, value, store, m0)

        def second_pass(x, sums):
            m1, m2 = sums
            r, d = spread(r_ref, x)
            w = r - implicit_diagonal * d
            return (m1 + fold(r * w), m2 + fold(w * w)), w

        def store_second(x, w):
            keep(w_tag, x, w)

        if step == 0:
            pass_on(1)
        with jax.named_scope("image"):
            sums = grouped("image", 1, nx - 1, second_pass, store_second, (nothing, nothing))

        def energy(x, low, rows):
            at, above = pl.ds(PAD + low, rows), pl.ds(PAD + low + 1, rows)
            mid = pl.ds(low, rows)
            w = w_ref[x + 1, at]
            jump_x = w_ref[x + 2, at] - w
            jump_y = w_ref[x + 1, above] - w
            jump_z = jnp.where(last_lane[:rows], 0.0, ahead_z(w)) - w
            total = cx[x + 1, mid] * jump_x * jump_x + cy[x, at] * jump_y * jump_y
            return fold(total + cz[x, mid] * jump_z * jump_z)

        with jax.named_scope("energy"):
            m3 = grouped("energy", 1, nx - 2, lambda x, m: (m + energy(x, 8, ny - 16), None), lambda x, kept: None, nothing)

        with jax.named_scope("arrive_y"):
            arrive(r_tag, YD, YU)
        with jax.named_scope("yfix"):
            unpack(r_tag)
            m1, m2 = sums
            for side, face in ((0, yrecv[7, 0]), (1, ysend[7, 1])):
                change = jnp.where(between, -implicit_diagonal * face * yrecv[r_tag, side], 0.0)
                w = ysend[w_tag, side]
                ysend[w_tag, side] = w + change
                m1 += fold(ysend[r_tag, side] * change)
                m2 += fold((2.0 * w + change) * change)
            for x in range(1, nx - 1):
                w_ref[1 + x, pl.ds(PAD, 1)] = ysend[w_tag, 0, pl.ds(x, 1)]
                w_ref[1 + x, pl.ds(PAD + ny - 1, 1)] = ysend[w_tag, 1, pl.ds(x, 1)]
        with jax.named_scope("rim"):
            m3 = grouped(
                "rim", 1, nx - 2, lambda x, m: (m + energy(x, 0, 8) + energy(x, ny - 8, 8), None), lambda x, kept: None, m3)
        with jax.named_scope("arrive_x"):
            arrive(r_tag, XD, XU)
        with jax.named_scope("edges"):
            sums = (m1, m2)
            for x in (0, nx - 1):
                sums, w = second_pass(x, sums)
                store_second(x, w)
            m1, m2 = sums
        with jax.named_scope("arrive_w"):
            arrive(w_tag, XD, YD)
            for copy, _, whence in corners(step):
                pl.when(whence)(copy.wait_recv)
        with jax.named_scope("close"):
            w_ref[nx + 1, own] = w_ref[nx + 1, own] - across_x * (cx[nx] * r_ref[nx, own])
            for k, y in ((0, 0), (1, ny - 1)):
                w_ref[nx + 1, pl.ds(PAD + y, 1)] -= implicit_diagonal * corner_in[step, k]
            above = yrecv[w_tag, 1] - across_y * (ysend[7, 1] * ysend[r_tag, 1])
            above -= jnp.where(row_x == 0, implicit_diagonal * corner_in[step, 3], 0.0)
            above -= jnp.where(row_x == nx - 1, implicit_diagonal * corner_in[step, 2], 0.0)
            for x in (0, nx - 2, nx - 1):
                m3 += energy(x, 0, ny)
            m3 += fold(ysend[7, 1] * above * (above - 2.0 * ysend[w_tag, 1]))
            m3 = m2 + implicit_diagonal * m3
        with jax.named_scope("sendsums"):
            if step == 0:
                pass_on(2, last=True)
            send_sums(step, (m0, m1, m2, m3))
            start(w_tag, YU, XU)
            for x in range(nx):
                w_ref[1 + x, pl.ds(PAD + ny, 1)] = above[x:x + 1]

        target = section - 1
        final = target == 0
        on_f, on_d = explicit_table[section][target], implicit_table[section][target]

        def carry(x, c):
            f = carried(r_ref, x)
            if final:
                r = r_ref[x + 1, own]
                f = on_f * f + ((on_d / implicit_diagonal) * (r - w_ref[x + 1, own]) + r)
            return c, f

        def store_r(x, kept):
            (out_r if final else fr[step])[x] = kept

        with jax.named_scope("carry"):
            grouped("carry", 0, nx, carry, store_r, 0)

        share = section_weights[target] / section_weights[3]

        def gather(x, c):
            total = share * fields[1][x + 1, own]
            for k in range(step):
                total += explicit_table[3 - k][target] * fr[k][x] + implicit_table[3 - k][target] * dw[k][x]
            if target == 0:
                total += fields[0][x + 1, own]
                for k in range(step):
                    on_r, on_w = weights[k]
                    total += on_r * fields[1 + k][x + 1, own] + on_w * fields[4 + k][x + 1, own]
            return c, total

        def store_base(x, kept):
            (out_base if final else base)[x] = kept

        with jax.named_scope("gather"):
            grouped("gather", 0, nx, gather, store_base, 0)

        def store_w(x, kept):
            if final:
                out_w[x] = kept
            else:
                fw[step][x], dw[step][x] = kept

        def both(x, c):
            f, (w, d) = carried(w_ref, x), spread(w_ref, x)
            return c, on_f * f + on_d * d + w if final else (f, d)

        with jax.named_scope("both"):
            grouped("both", 1, nx, both, store_w, 0)
        with jax.named_scope("arrive_up"):
            arrive(w_tag, XU, YU)
        with jax.named_scope("late"):
            w_ref[1, pl.ds(PAD - 1, 1)] = yrecv[w_tag, 0, pl.ds(0, 1)]
            store_w(0, both(0, 0)[1])
            head = pl.ds(0, 1)
            owed_f = yrecv[8, 0] * yrecv[w_tag, 0]
            owed_d = yrecv[7, 0] * yrecv[w_tag, 0]
            owed = on_f * owed_f + on_d * owed_d
            for x in range(1, nx):
                if final:
                    out_w[x, head] += owed[x:x + 1]
                else:
                    fw[step][x, head] += owed_f[x:x + 1]
                    dw[step][x, head] += owed_d[x:x + 1]

        with jax.named_scope("allsums"):
            m0, m1, m2, m3 = read_sums(step)
        alpha = m0 / m1
        beyond = m1 / m0
        rr = alpha * alpha * m2 - m0
        ratio = rr * (1.0 / m0)
        product = m1 - 2.0 * alpha * m2 + alpha * alpha * m3
        alpha_next = rr / (product - ratio * rr * beyond)
        on_r = alpha + alpha_next * (1.0 + ratio)
        on_w = -alpha_next * alpha
        weights.append((on_r, on_w))

        def following(x, low, rows, step=step, on_r=on_r, on_w=on_w, on_f=on_f, on_d=on_d):
            at, mid = pl.ds(PAD + low, rows), pl.ds(low, rows)
            r, w = fields[1 + step][x + 1, at], fields[4 + step][x + 1, at]
            advected = on_r * fr[step][x, mid] + on_w * fw[step][x, mid]
            diffused = (on_r / implicit_diagonal) * (r - w) + on_w * dw[step][x, mid]
            total = base[x, mid]
            total += on_f * advected + on_d * diffused
            return total, (advected, diffused)

    out_scale[...] = jnp.concatenate(weights[-1], axis=0)
    with jax.named_scope("sends"):
        for xu, yu in statics:
            pl.when(high_x)(xu.wait_send)
            pl.when(high_y)(yu.wait_send)
        for tag in range(7):
            sent(tag)
        for step in range(3):
            for copy, toward, _ in corners(step):
                pl.when(toward)(copy.wait_send)
            all_sums(step).wait_send()


def finish(base, on_r, on_w, scale, out_hbm, out, sem):
    nx = base.shape[0]
    chunks = CHUNKS if nx % CHUNKS == 0 else 1
    piece = nx // chunks
    copies = []
    for chunk in range(chunks):
        at = pl.ds(chunk * piece, piece)
        for x in range(chunk * piece, (chunk + 1) * piece):
            out[x] = base[x] + scale[:1] * on_r[x] + scale[1:] * on_w[x]
        copies.append(pltpu.make_async_copy(out.at[at], out_hbm.at[at], sem.at[chunk]))
        copies[-1].start()
    for copy in copies:
        copy.wait()


def local(gx, gy, cotangent, speed, coeff, dirs):
    nx, ny, nz = cotangent.shape
    f32 = jnp.float32
    rows = ny + 2 * PAD
    plain = pltpu.VMEM((nx, ny, nz), f32)
    dma = pltpu.SemaphoreType.DMA
    far = pl.BlockSpec(memory_space=pltpu.HBM)
    hbm = [pltpu.with_memory_space_constraint(v, pltpu.HBM) for v in (cotangent, speed, coeff, dirs)]
    whole = jax.ShapeDtypeStruct((nx, ny, nz), f32)
    total, on_r, on_w, scale = pl.pallas_call(
        functools.partial(kernel, gx, gy),
        out_shape=(whole, whole, whole, jax.ShapeDtypeStruct((2, nz), f32)),
        in_specs=[far] * 4,
        out_specs=(pl.BlockSpec(memory_space=pltpu.VMEM),) * 4,
        scratch_shapes=[
            *[pltpu.VMEM((nx + 2, rows, nz), f32)] * 7,
            *[plain] * 6,
            plain,
            pltpu.VMEM((nx + 1, ny, nz), f32),
            pltpu.VMEM((nx, rows, nz), f32),
            plain, plain,
            plain, plain, plain,
            pltpu.VMEM((nx + 1, ny, nz), f32),
            pltpu.VMEM((nx, rows, nz), f32),
            plain,
            plain, plain,
            pltpu.VMEM((9, 2, nx, nz), f32),
            pltpu.VMEM((9, 2, nx, nz), f32),
            pltpu.VMEM(dirs.shape, dirs.dtype),
            pltpu.VMEM((2, ny, nz), f32),
            pltpu.VMEM((ny, nz), f32),
            pltpu.VMEM((ny, nz), f32),
            pltpu.VMEM((nx, 8, nz), f32),
            pltpu.VMEM((nx, 8, nz), f32),
            pltpu.VMEM((2, ny, nz), f32),
            pltpu.VMEM((3, ny, nz), f32),
            pltpu.VMEM((3, nx, nz), f32),
            pltpu.VMEM((7, nx, nz), f32),
            pltpu.VMEM((3, 4, 1, nz), f32),
            pltpu.VMEM((3, 4, 1, nz), f32),
            pltpu.VMEM((3, gx * gy, 1, nz), f32),
            dma((8 + 6 * CHUNKS,)), dma((9, 4)), dma((9, 4)),
            dma((3, 3)), dma((3, 3)), dma((3,)), dma((3,)),
            pltpu.SemaphoreType.REGULAR((max(gx, gy).bit_length(),)),
        ],
        compiler_params=pltpu.CompilerParams(
            collective_id=0, has_side_effects=True, vmem_limit_bytes=46 * 1024 * 1024
        ),
    )(*hbm)
    return pl.pallas_call(
        finish,
        out_shape=whole,
        in_specs=[pl.BlockSpec(memory_space=pltpu.VMEM)] * 4,
        out_specs=pl.BlockSpec(memory_space=pltpu.HBM),
        scratch_shapes=[plain, dma((CHUNKS,))],
        compiler_params=pltpu.CompilerParams(vmem_limit_bytes=8 * 1024 * 1024),
    )(total, on_r, on_w, scale)


def solution(mesh):
    return jax.shard_map(
        functools.partial(local, mesh.shape["gx"], mesh.shape["gy"]),
        mesh=mesh,
        in_specs=(
            P("gx", "gy", None),
            P(None, "gx", "gy", None),
            P(None, "gx", "gy", None),
            P(None, "gx", "gy"),
        ),
        out_specs=P("gx", "gy", None),
        check_vma=False,
    )
```
